768 devices in a mesh: ta: 16 (over y, x_lo), gz: 4 (over x_hi, core), xy: 12 (over z).
Axes of the slice: x: 4 (x_hi: 2, x_lo: 2; x = x_hi * 2 + x_lo), y: 8, z: 12, core: 2. Of those that a mesh axis runs over, the one named last changes fastest.
Arguments:
- source_field: float32 [2, 4, 3, 16, 4, 12, 128], P(None, None, None, 'ta', 'gz', 'xy'), may hold values from -6 to 6
- gauge_links: float32 [2, 8, 3, 3, 16, 4, 12, 128], P(None, None, None, None, 'ta', 'gz', 'xy'), may hold values from -2.5 to 2.5
- fine_vectors: bfloat16 [2, 24, 4, 3, 16, 4, 12, 128], P(None, None, None, None, 'ta', 'gz', 'xy'), may hold values from -1.75 to 1.75
- middle_blocks: float32 [2, 9, 24, 16, 4, 12, 768], P(None, None, None, 'ta', 'gz', 'xy'), may hold values from -0.3125 to 0.3125
- middle_vectors: float32 [2, 24, 16, 4, 12, 768], P(None, None, 'ta', 'gz', 'xy'), may hold values from -0.625 to 0.625
- bottom_blocks: float32 [2, 7, 16, 4, 6912], P(None, None, 'ta', 'gz'), may hold values from -4 to 4
Outputs:
- solution: float32 [2, 4, 3, 16, 4, 12, 128], P(None, None, None, 'ta', 'gz', 'xy')
- smoothed_residual: float32 [2, 4, 3, 16, 4, 12, 128], P(None, None, None, 'ta', 'gz', 'xy')
The draws below stay inside these ranges and needn't reach their ends.
All inputs are finite; a program needn't handle non-finite values.
Results may differ from the reference program's by a relative error of at most 0.0034.
Values sent between devices are 32-bit elements; how exact they have to be, the bound alone decides.
A program may use at most 64 MiB of HBM per device.

```python
import math
import jax
import jax.numpy as jnp
import numpy as np
from jax import lax

TL = 1
ZL = 1
XL = 1
YL = 128
BY = 4
NVEC = 24
NVEC2 = 24
YBLOCKS = 32
NT = 16
NZ = 4
NX = 12
N_TA = 16
N_GZ = 4
N_XY = 12


def draw_bottom_blocks(key, part):
    shape_list = (2, 7, NVEC2, NVEC2, N_TA, N_GZ, N_XY)
    entries = jax.random.normal(jax.random.fold_in(key, 11), shape_list, jnp.float32)
    spread = jnp.exp(jax.random.uniform(jax.random.fold_in(key, 13), (N_TA, N_GZ, N_XY), jnp.float32, -1.2, 1.2))
    rising = 3.0 ** (jnp.arange(N_TA, dtype=jnp.float32) / max(N_TA - 1, 1))
    scaling = spread * rising[:, None, None] / math.sqrt(14.0 * NVEC2)
    blocks = jnp.clip(entries * scaling, -4.0, 4.0)
    ordered = jnp.transpose(blocks, (0, 1, 4, 5, 6, 2, 3))
    return ordered.reshape((2, 7, N_TA, N_GZ, N_XY * NVEC2 * NVEC2))


def level_of(stream_key, dims, cuts, smallest, top_value):
    loudness, own = 1.0, jax.random.fold_in(stream_key, 6)
    for position, shards_of in cuts:
        draws = jnp.exp(jax.random.uniform(jax.random.fold_in(own, position), (shards_of,), jnp.float32, smallest / len(cuts), top_value / len(cuts)))
        loudness = loudness * jnp.repeat(draws, dims[position] // shards_of).reshape([-1 if axis == position else 1 for axis in range(len(dims))])
    return loudness


def bell_draw(own_key, dims, scale, limit, pieces=(), kind=jnp.bfloat16):
    level = level_of(own_key, dims, pieces, -0.22, 0.18) if pieces else 1.0
    drawn = jax.random.normal(own_key, dims, jnp.float32) * scale * level
    return jnp.minimum(jnp.maximum(drawn, -limit), limit).astype(kind)


def setup_inputs(seed: int = 0) -> dict:
    seeds = jax.random.split(jax.random.key(seed), 7)
    return {
        "source_field": bell_draw(seeds[0], (2, 4, 3, NT, NZ, NX, YL), 1.0, 6.0, ((3, 16), (4, 4), (5, 12)), jnp.float32),
        "gauge_links": bell_draw(seeds[1], (2, 8, 3, 3, NT, NZ, NX, YL), 6 ** -0.5, 2.5, ((4, 16), (5, 4), (6, 12)), jnp.float32),
        "fine_vectors": bell_draw(seeds[2], (2, NVEC, 4, 3, NT, NZ, NX, YL), (TL * ZL * XL * BY * 3) ** -0.5, 1.75, ((4, 16), (5, 4), (6, 12))),
        "middle_blocks": bell_draw(seeds[3], (2, 9, NVEC, N_TA, N_GZ, N_XY, NVEC * YBLOCKS), (18 * NVEC) ** -0.5, 0.3125, ((3, 16), (4, 4), (5, 12)), jnp.float32),
        "middle_vectors": bell_draw(seeds[4], (2, NVEC2, N_TA, N_GZ, N_XY, NVEC * YBLOCKS), (4 * NVEC) ** -0.5, 0.625, ((2, 16), (3, 4), (4, 12)), jnp.float32),
        "bottom_blocks": draw_bottom_blocks(jax.random.fold_in(seeds[6], 71), 0),
    }


quark_mass = 0.1
twist_mass = 0.1
fine_damping = 0.8
middle_damping = 0.4
middle_shift = 2.0
bottom_shift = 2.0

gamma_real = np.array([
    [[0, 0, 1, 0], [0, 0, 0, 1], [1, 0, 0, 0], [0, 1, 0, 0]],
    [[0] * 4] * 4,
    [[0] * 4] * 4,
    [[0, 0, 0, -1], [0, 0, 1, 0], [0, 1, 0, 0], [-1, 0, 0, 0]]], np.float32)
gamma_imag = np.array([
    [[0] * 4] * 4,
    [[0, 0, 1, 0], [0, 0, 0, -1], [-1, 0, 0, 0], [0, 1, 0, 0]],
    [[0, 0, 0, 1], [0, 0, 1, 0], [0, -1, 0, 0], [-1, 0, 0, 0]],
    [[0] * 4] * 4], np.float32)
chirality = np.array([1.0, 1.0, -1.0, -1.0], np.float32)


def color_apply(link_pair, spinor):
    link_re = link_pair[0][None]
    link_im = link_pair[1][None]
    part_re = spinor[0][:, None]
    part_im = spinor[1][:, None]
    real_part = jnp.sum(link_re * part_re - link_im * part_im, axis=2)
    imag_part = jnp.sum(link_re * part_im + link_im * part_re, axis=2)
    return jnp.stack([real_part, imag_part])


def apply_table(table_value, part_value):
    return jnp.tensordot(jnp.asarray(table_value), part_value, axes=([1], [0]), precision=lax.Precision.HIGHEST)


def spin_mix(spinor, direction):
    real_part = apply_table(gamma_real[direction], spinor[0]) - apply_table(gamma_imag[direction], spinor[1])
    imag_part = apply_table(gamma_real[direction], spinor[1]) + apply_table(gamma_imag[direction], spinor[0])
    return jnp.stack([real_part, imag_part])


def chirality_sign(spinor):
    return jnp.asarray(chirality).reshape((4,) + (1,) * (spinor.ndim - 2))


def twisted_diagonal(spinor):
    signs = chirality_sign(spinor)
    diagonal_value = 4.0 + quark_mass
    real_part = diagonal_value * spinor[0] - twist_mass * signs * spinor[1]
    imag_part = diagonal_value * spinor[1] + twist_mass * signs * spinor[0]
    return jnp.stack([real_part, imag_part])


def precondition(spinor):
    signs = chirality_sign(spinor)
    diagonal_value = 4.0 + quark_mass
    denominator = diagonal_value * diagonal_value + twist_mass * twist_mass
    real_part = (diagonal_value * spinor[0] + twist_mass * signs * spinor[1]) / denominator
    imag_part = (diagonal_value * spinor[1] - twist_mass * signs * spinor[0]) / denominator
    return jnp.stack([real_part, imag_part])


def wilson(spinor, ahead_list, behind_list, gauge_links):
    hopping = jnp.zeros_like(spinor)
    for direction in range(4):
        upward = color_apply(gauge_links[:, 2 * direction], ahead_list[direction])
        downward = color_apply(gauge_links[:, 2 * direction + 1], behind_list[direction])
        hopping = hopping + upward - spin_mix(upward, direction) + downward + spin_mix(downward, direction)
    return twisted_diagonal(spinor) - 0.5 * hopping


def fine_operator(spinor, gauge_links):
    ahead_list = [jnp.roll(spinor, -1, axis=3 + direction) for direction in range(4)]
    behind_list = [jnp.roll(spinor, 1, axis=3 + direction) for direction in range(4)]
    return wilson(spinor, ahead_list, behind_list, gauge_links)


def middle_layout(blocks):
    count = blocks.shape[2]
    split = blocks.reshape(blocks.shape[:6] + (count, blocks.shape[6] // count))
    return jnp.moveaxis(split, 6, 3)


def vector_layout(vectors):
    split = vectors.reshape(vectors.shape[:5] + (NVEC, vectors.shape[5] // NVEC))
    return jnp.moveaxis(split, 5, 2)


def bottom_layout(blocks):
    split = blocks.reshape(blocks.shape[:4] + (-1, NVEC2, NVEC2))
    return jnp.transpose(split, (0, 1, 5, 6, 2, 3, 4))


def block_apply(blocks, near_stack):
    def block_product(matrix, vector):
        return jnp.einsum('djk...,dk...->j...', matrix, vector, precision=lax.Precision.HIGHEST)
    real_part = block_product(blocks[0], near_stack[0]) - block_product(blocks[1], near_stack[1])
    imag_part = block_product(blocks[0], near_stack[1]) + block_product(blocks[1], near_stack[0])
    return jnp.stack([real_part, imag_part])


def restrict_middle(middle_vectors, coarse):
    def contract(left_side, right_side):
        return jnp.einsum('kjtzxa,jtzxa->ktzx', left_side, right_side, precision=lax.Precision.HIGHEST)
    real_part = contract(middle_vectors[0], coarse[0]) + contract(middle_vectors[1], coarse[1])
    imag_part = contract(middle_vectors[0], coarse[1]) - contract(middle_vectors[1], coarse[0])
    return jnp.stack([real_part, imag_part])


def prolong_middle(middle_vectors, coarse):
    def contract(left_side, right_side):
        return jnp.einsum('kjtzxa,ktzx->jtzxa', left_side, right_side, precision=lax.Precision.HIGHEST)
    real_part = contract(middle_vectors[0], coarse[0]) - contract(middle_vectors[1], coarse[1])
    imag_part = contract(middle_vectors[0], coarse[1]) + contract(middle_vectors[1], coarse[0])
    return jnp.stack([real_part, imag_part])


def inner_product(left_side, right_side):
    real_part = jnp.sum(left_side[0] * right_side[0] + left_side[1] * right_side[1])
    imag_part = jnp.sum(left_side[0] * right_side[1] - left_side[1] * right_side[0])
    return real_part, imag_part


def gram_partials(right_side, first_image, second_image):
    first_norm = inner_product(first_image, first_image)[0]
    second_norm = inner_product(second_image, second_image)[0]
    cross_re, cross_im = inner_product(first_image, second_image)
    first_re, first_im = inner_product(first_image, right_side)
    second_re, second_im = inner_product(second_image, right_side)
    return jnp.stack([first_norm, second_norm, cross_re, cross_im, first_re, first_im, second_re, second_im])


def complex_scale(coef_re, coef_im, vector):
    return jnp.stack([coef_re * vector[0] - coef_im * vector[1], coef_re * vector[1] + coef_im * vector[0]])


def least_squares(totals, right_side, first_image):
    first_norm = totals[0]
    second_norm = totals[1]
    cross_re = totals[2]
    cross_im = totals[3]
    first_re = totals[4]
    first_im = totals[5]
    second_re = totals[6]
    second_im = totals[7]
    determinant = first_norm * second_norm - cross_re * cross_re - cross_im * cross_im
    coef_one_re = (second_norm * first_re - (cross_re * second_re - cross_im * second_im)) / determinant
    coef_one_im = (second_norm * first_im - (cross_re * second_im + cross_im * second_re)) / determinant
    coef_two_re = (first_norm * second_re - (cross_re * first_re + cross_im * first_im)) / determinant
    coef_two_im = (first_norm * second_im - (cross_re * first_im - cross_im * first_re)) / determinant
    return complex_scale(coef_one_re, coef_one_im, right_side) + complex_scale(coef_two_re, coef_two_im, first_image)


def restrict_fine(residual_low, fine_vectors):
    split_vectors = fine_vectors.reshape((2, NVEC, 4, 3, N_TA, TL, N_GZ, ZL, N_XY, XL, YBLOCKS, BY))
    split_residual = residual_low.reshape((2, 4, 3, N_TA, TL, N_GZ, ZL, N_XY, XL, YBLOCKS, BY))
    collected = []
    for block in range(YBLOCKS):
        piece_vectors = split_vectors[..., block, :].astype(jnp.float32)
        piece_residual = split_residual[..., block, :].astype(jnp.float32)
        collected.append(jnp.einsum('pkscdefghib,qscdefghib->pqkdfh', piece_vectors, piece_residual,
                                    precision=lax.Precision.HIGHEST))
    terms = jnp.stack(collected, axis=-1)
    return jnp.stack([terms[0, 0] + terms[1, 1], terms[0, 1] - terms[1, 0]])


def prolong_fine(update_low, fine_vectors):
    split_vectors = fine_vectors.reshape((2, NVEC, 4, 3, N_TA, TL, N_GZ, ZL, N_XY, XL, YBLOCKS, BY))
    collected = []
    for block in range(YBLOCKS):
        piece_vectors = split_vectors[..., block, :].astype(jnp.float32)
        coefficients = update_low[..., block].astype(jnp.float32)
        terms = jnp.einsum('pkscdefghib,qkdfh->pqscdefghib', piece_vectors, coefficients,
                           precision=lax.Precision.HIGHEST)
        collected.append(jnp.stack([terms[0, 0] - terms[1, 1], terms[0, 1] + terms[1, 0]]))
    joined = jnp.stack(collected, axis=-2)
    return joined.reshape((2, 4, 3, NT, NZ, NX, YL))


def middle_operator(coarse, middle_blocks):
    near_list = [coarse]
    for axis_number in (2, 3, 4, 5):
        near_list.append(jnp.roll(coarse, -1, axis=axis_number))
        near_list.append(jnp.roll(coarse, 1, axis=axis_number))
    return middle_shift * coarse + block_apply(middle_blocks, jnp.stack(near_list, axis=1))


def bottom_operator(coarse, bottom_blocks):
    near_list = [coarse]
    for axis_number in (2, 3, 4):
        near_list.append(jnp.roll(coarse, -1, axis=axis_number))
        near_list.append(jnp.roll(coarse, 1, axis=axis_number))
    return bottom_shift * coarse + block_apply(bottom_blocks, jnp.stack(near_list, axis=1))


def reference(source_field, gauge_links, fine_vectors, middle_blocks, middle_vectors, bottom_blocks):
    middle_blocks = middle_layout(middle_blocks)
    middle_vectors = vector_layout(middle_vectors)
    bottom_blocks = bottom_layout(bottom_blocks)
    first_iterate = fine_damping * precondition(source_field)
    first_residual = source_field - fine_operator(first_iterate, gauge_links)
    second_iterate = first_iterate + fine_damping * precondition(first_residual)
    smoothed_residual = source_field - fine_operator(second_iterate, gauge_links)
    middle_right = restrict_fine(smoothed_residual.astype(jnp.bfloat16), fine_vectors)
    bottom_right = restrict_middle(middle_vectors, middle_right)
    first_image = bottom_operator(bottom_right, bottom_blocks)
    second_image = bottom_operator(first_image, bottom_blocks)
    totals = gram_partials(bottom_right, first_image, second_image)
    bottom_solution = least_squares(totals, bottom_right, first_image)
    middle_guess = prolong_middle(middle_vectors, bottom_solution)
    middle_update = middle_guess + middle_damping * (middle_right - middle_operator(middle_guess, middle_blocks))
    correction = prolong_fine(middle_update.astype(jnp.bfloat16), fine_vectors)
    return second_iterate + correction, smoothed_residual
```

```python
import functools

import jax
import jax.numpy as jnp
import numpy as np
from jax import lax
from jax.experimental import pallas as pl
from jax.experimental.pallas import tpu as pltpu
from jax.sharding import PartitionSpec as P

MESH = pl.DeviceIdType.MESH
F32 = jnp.float32
BF16 = jnp.bfloat16

DIAGONAL = 4.1
TWIST = 0.1
DENOMINATOR = DIAGONAL * DIAGONAL + TWIST * TWIST
PRE_SAME = 0.8 * DIAGONAL / DENOMINATOR
PRE_OTHER = 0.8 * TWIST / DENOMINATOR

STEPS = ((1, 0, 0), (-1, 0, 0), (0, 1, 0), (0, -1, 0), (0, 0, 1), (0, 0, -1))
NEAR = ((0, 0, 0),) + STEPS


def added(one, other):
    return tuple(a + b for a, b in zip(one, other))


def plan(sizes):
    def wrapped(offset):
        return tuple(o % n for o, n in zip(offset, sizes))

    slots = {}
    for one in NEAR:
        for other in NEAR:
            slots.setdefault(wrapped(added(one, other)), len(slots))
    plane = {}
    for dt in range(sizes[0]):
        for dz in range(sizes[1]):
            plane[(dt, dz, 0)] = len(plane)
    line = {(0, 0, dx): dx for dx in range(sizes[2])}
    peers = set(slots) | set(plane) | set(line)
    peers.discard((0, 0, 0))
    return wrapped, slots, plane, line, sorted(peers)


def tables():
    lane = np.arange(128)
    spread = np.zeros((128, 1280), np.float32)
    collect = np.zeros((640, 128), np.float32)
    for j in range(24):
        for k in range(24):
            spread[k, j * 24 + k] = 1
            spread[32 + k, 640 + j * 24 + k] = 1
            collect[j * 24 + k, j] = 1
    unfold = (lane[:, None] % 32 == lane[None] // 4).astype(np.float32)
    share = (lane[:, None] // 4 == lane[None] // 4).astype(np.float32)
    square = np.concatenate([unfold, unfold.T, share], 0)
    return spread, collect, square


def pieces(value):
    high = value.astype(BF16)
    rest = value - high.astype(F32)
    middle = rest.astype(BF16)
    low = (rest - middle.astype(F32)).astype(BF16)
    return high, middle, low


def times_table(value, table):
    high, middle, low = pieces(value)
    return (
        jnp.dot(high, table, preferred_element_type=F32)
        + jnp.dot(middle, table, preferred_element_type=F32)
        + jnp.dot(low, table, preferred_element_type=F32)
    )


def row_sums(value):
    ones = jnp.ones((8, 128), BF16)
    dims = (((1,), (1,)), ((), ()))
    return sum(
        lax.dot_general(ones, piece, dims, preferred_element_type=F32) for piece in pieces(value)
    )


def kernel(
    sizes,
    src_h, gauge_h, fine_h, mblk_h, mvec_h, bblk_h, spread_h, collect_h, square_h,
    sol_ref, res_ref,
    src, gauge, fine, mblk, mvec, bblk, spread, collect, square,
    halo, hop_rows, second, fine_f, mv_parts, own_blk, got_blk, near_blk,
    right_rows, sum_rows, around, spread_rows, gram_rows, plane_rows, line_rows, mid, wide, final,
    local_sem, halo_send, halo_recv, blk_send, blk_recv, right_send, right_recv,
    plane_send, plane_recv, line_send, line_recv, mid_send, mid_recv,
):
    wrapped, slots, plane, line, peers = plan(sizes)
    here = tuple(lax.axis_index(axis) for axis in ("ta", "gz", "xy"))

    def at(offset):
        return tuple(
            h if o % n == 0 else lax.rem(h + (o % n), n) for h, o, n in zip(here, offset, sizes)
        )

    def against(offset):
        return at(tuple(-o for o in offset))

    loads = [
        pltpu.make_async_copy(a, b, local_sem.at[i])
        for i, (a, b) in enumerate(
            (
                (src_h, src), (gauge_h, gauge), (bblk_h, bblk), (fine_h, fine), (mvec_h, mvec),
                (spread_h, spread), (collect_h, collect), (square_h, square), (mblk_h, mblk),
            )
        )
    ]
    for load in loads:
        load.start()

    barrier = pltpu.get_barrier_semaphore()
    for offset in peers:
        pl.semaphore_signal(barrier, inc=1, device_id=at(offset), device_id_type=MESH)

    def remote(source, target, send, recv, device):
        return pltpu.make_async_remote_copy(
            src_ref=source, dst_ref=target, send_sem=send, recv_sem=recv,
            device_id=device, device_id_type=MESH,
        )

    def halo_copies(source, which):
        return [
            remote(
                source, halo.at[which, d], halo_send.at[which, d], halo_recv.at[which, d],
                against(STEPS[d]),
            )
            for d in range(6)
        ]

    loads[0].wait()
    pl.semaphore_wait(barrier, len(peers))
    first_copies = halo_copies(src, 0)
    for copy in first_copies:
        copy.start()

    lanes8 = lax.broadcasted_iota(jnp.int32, (8, 128), 1)
    low_half = lanes8 < 64
    near_blk[...] = jnp.zeros_like(near_blk)
    own_blk[...] = jnp.zeros_like(own_blk)
    around[...] = jnp.zeros_like(around)
    sum_rows[...] = jnp.zeros_like(sum_rows)
    gram_rows[...] = jnp.zeros_like(gram_rows)
    mv_parts[...] = jnp.zeros_like(mv_parts)
    loads[2].wait()
    per_x = bblk.shape[0] // 14

    def site_blocks(x):
        start = (x * 9) // 2
        odd = lax.rem(x, 2) == 1
        for p in range(2):
            chunks = [
                bblk[pl.ds(p * 7 * per_x + start + q, 7, stride=per_x), 0, :] for q in range(5)
            ]
            for q in range(5):
                here_now = chunks[q]
                after = chunks[min(q + 1, 4)]
                moved = jnp.where(
                    low_half[:7], pltpu.roll(here_now, 64, 1), pltpu.roll(after, 64, 1)
                )
                yield p, q, jnp.where(odd, moved, here_now)

    for p, q, value in site_blocks(here[2]):
        own_blk[p, q, pl.ds(0, 7), :] = value
        near_blk[p, q, pl.ds(0, 7, stride=8), :] = value
    blk_copies = [
        remote(own_blk, got_blk.at[d], blk_send.at[d], blk_recv.at[d], against(STEPS[d]))
        for d in range(4)
    ]
    for copy in blk_copies:
        copy.start()
    for d in (4, 5):
        for p, q, value in site_blocks(at(STEPS[d])[2]):
            near_blk[p, q, pl.ds(1 + d, 7, stride=8), :] = value
    loads[3].wait()
    fine_f[...] = fine[...].astype(F32)
    loads[4].wait()
    for p in range(2):
        for c in range(6):
            block = mvec[pl.ds(p * 144 + c, 24, stride=6), :]
            high = block.astype(BF16)
            mv_parts[p, 0, pl.ds(0, 24), pl.ds(c * 128, 128)] = high
            mv_parts[p, 1, pl.ds(0, 24), pl.ds(c * 128, 128)] = (block - high.astype(F32)).astype(BF16)

    direction = lax.broadcasted_iota(jnp.int32, (8, 128), 0)
    is_t = direction < 2
    is_z = direction < 4
    is_x = direction < 6
    odd_one = lax.rem(direction, 2) == 1
    base = jnp.where(odd_one, 1.0, -1.0).astype(F32)
    in_z = jnp.logical_and(is_z, jnp.logical_not(is_t))
    in_x = jnp.logical_and(is_x, jnp.logical_not(is_z))
    in_y = jnp.logical_not(is_x)

    def flipped(mask):
        return jnp.where(mask, -base, base)

    sign_a = flipped(jnp.logical_not(is_t))
    sign_b = flipped(in_y)
    sign_c = flipped(in_x)
    sign_d = flipped(in_z)
    sign_e = flipped(jnp.logical_or(in_z, in_x))
    sign_f = flipped(jnp.logical_or(in_z, in_y))
    sign_g = flipped(jnp.logical_or(in_x, in_y))

    def pick(a, b, c, d):
        return jnp.where(is_t, a, jnp.where(is_z, b, jnp.where(is_x, c, d)))

    loads[1].wait()

    def hopping(near):
        link = [
            [[gauge[pl.ds(p * 72 + c * 3 + e, 8, stride=9), :] for e in range(3)] for c in range(3)]
            for p in range(2)
        ]
        (r0, r1, r2, r3), (i0, i1, i2, i3) = near
        half = [[[None] * 3 for _ in range(2)] for _ in range(2)]
        for c in range(3):
            half[0][0][c] = r0[c] + sign_a * pick(r2[c], i2[c], i3[c], r3[c])
            half[1][0][c] = i0[c] + sign_b * pick(i2[c], r2[c], r3[c], i3[c])
            half[0][1][c] = r1[c] + sign_c * pick(r3[c], i3[c], i2[c], r2[c])
            half[1][1][c] = i1[c] + sign_d * pick(i3[c], r3[c], r2[c], i2[c])

        def put(p, s, c, value):
            hop_rows[pl.ds(p * 12 + s * 3 + c, 1), :] = jnp.sum(value, axis=0, keepdims=True)

        for c in range(3):
            moved = [[0.0, 0.0], [0.0, 0.0]]
            for s in range(2):
                for e in range(3):
                    lr, li = link[0][c][e], link[1][c][e]
                    hr, hi = half[0][s][e], half[1][s][e]
                    moved[0][s] = moved[0][s] + (lr * hr - li * hi)
                    moved[1][s] = moved[1][s] + (lr * hi + li * hr)
            (a0, a1), (b0, b1) = moved
            put(0, 0, c, a0)
            put(0, 1, c, a1)
            put(1, 0, c, b0)
            put(1, 1, c, b1)
            put(0, 2, c, base * pick(a0, b0, b1, a1))
            put(1, 2, c, sign_e * pick(b0, a0, a1, b1))
            put(0, 3, c, sign_f * pick(a1, b1, b0, a0))
            put(1, 3, c, sign_g * pick(b1, a1, a0, b0))

    def near_values(which):
        return [
            [
                [halo[which, :, p * 12 + s * 3 + c, :] for c in range(3)]
                for s in range(4)
            ]
            for p in range(2)
        ]

    def fill_y(which, field):
        halo[which, 6] = pltpu.roll(field, 127, 1)
        halo[which, 7] = pltpu.roll(field, 1, 1)

    rows12 = lax.broadcasted_iota(jnp.int32, (12, 128), 0)
    chiral = jnp.where(rows12 < 6, 1.0, -1.0).astype(F32)

    def smoothed(re, im):
        return (
            PRE_SAME * re + PRE_OTHER * (chiral * im),
            PRE_SAME * im - PRE_OTHER * (chiral * re),
        )

    def residual(re, im):
        hop_re, hop_im = hop_rows[0:12, :], hop_rows[12:24, :]
        out_re = src[0:12, :] - (DIAGONAL * re - TWIST * (chiral * im) - 0.5 * hop_re)
        out_im = src[12:24, :] - (DIAGONAL * im + TWIST * (chiral * re) - 0.5 * hop_im)
        return out_re, out_im

    fill_y(0, src[...])
    for copy in first_copies:
        copy.wait_recv()
    raw = near_values(0)
    ready = [[[None] * 3 for _ in range(4)] for _ in range(2)]
    for s in range(4):
        other = PRE_OTHER if s < 2 else -PRE_OTHER
        for c in range(3):
            re, im = raw[0][s][c], raw[1][s][c]
            ready[0][s][c] = PRE_SAME * re + other * im
            ready[1][s][c] = PRE_SAME * im - other * re
    hopping(ready)
    first_re, first_im = smoothed(src[0:12, :], src[12:24, :])
    left_re, left_im = smoothed(*residual(first_re, first_im))
    second_re, second_im = first_re + left_re, first_im + left_im
    second[0:12, :] = second_re
    second[12:24, :] = second_im
    second_copies = halo_copies(second, 1)
    for copy in second_copies:
        copy.start()

    for d in range(4):
        blk_copies[d].wait_recv()
        for p in range(2):
            for q in range(5):
                near_blk[p, q, pl.ds(1 + d, 7, stride=8), :] = got_blk[d, p, q, pl.ds(0, 7), :]
    for load in loads[5:8]:
        load.wait()

    fill_y(1, second[...])
    for copy in second_copies:
        copy.wait_recv()
    hopping(near_values(1))
    res_re, res_im = residual(second_re, second_im)
    res_ref[0:12, :] = res_re
    res_ref[12:24, :] = res_im
    hop_rows[0:12, :] = res_re.astype(BF16).astype(F32)
    hop_rows[12:24, :] = res_im.astype(BF16).astype(F32)

    def fine_vector(p, s, c):
        return fine_f[pl.ds(p * 288 + c * 4 + s, 24, stride=12), :]

    part_re = jnp.zeros((24, 128), F32)
    part_im = jnp.zeros((24, 128), F32)
    for s in range(4):
        for c in range(3):
            vr, vi = fine_vector(0, s, c), fine_vector(1, s, c)
            rr = hop_rows[pl.ds(s * 3 + c, 1), :]
            ri = hop_rows[pl.ds(12 + s * 3 + c, 1), :]
            part_re = part_re + (vr * rr + vi * ri)
            part_im = part_im + (vr * ri - vi * rr)
    parts = jnp.concatenate([part_re, part_im], axis=0)
    wide[0:48, :] = times_table(parts, square[128:256, :])
    lane_row = lax.broadcasted_iota(jnp.int32, (1, 128), 1)

    def middle_row(p, c):
        rows = [wide[pl.ds(p * 24 + c * 4 + g, 1), :] for g in range(4)]
        return jnp.where(
            lane_row < 64,
            jnp.where(lane_row < 32, rows[0], rows[1]),
            jnp.where(lane_row < 96, rows[2], rows[3]),
        )

    q_re = jnp.zeros((24, 128), F32)
    q_im = jnp.zeros((24, 128), F32)
    for c in range(6):
        vr = mvec[pl.ds(c, 24, stride=6), :]
        vi = mvec[pl.ds(144 + c, 24, stride=6), :]
        mr, mi = middle_row(0, c), middle_row(1, c)
        q_re = q_re + (vr * mr + vi * mi)
        q_im = q_im + (vr * mi - vi * mr)
    sum_rows[0:24, :] = q_re
    sum_rows[32:56, :] = q_im
    right_rows[pl.ds(0, 1)] = row_sums(sum_rows[...])[0:1].reshape(1, 1, 128)

    right_copies = [
        remote(
            right_rows.at[0], right_rows.at[slot], right_send.at[slot], right_recv.at[slot],
            against(offset),
        )
        for offset, slot in slots.items()
        if slot
    ]
    for copy in right_copies:
        copy.start()
    final[pl.ds(96, 48), :] = 0.4 * times_table(parts, square[256:384, :])
    for copy in right_copies:
        copy.wait_recv()

    for d in range(7):
        for i in range(7):
            slot = slots[wrapped(added(NEAR[d], NEAR[i]))]
            around[pl.ds(d * 8 + i, 1), :] = right_rows[slot]
    spread_rows[...] = times_table(around[...], spread[...])
    image_re, image_im = [], []
    for q in range(5):
        sum_re = jnp.zeros((8, 128), F32)
        sum_im = jnp.zeros((8, 128), F32)
        for d in range(7):
            br = near_blk[0, q, pl.ds(d * 8, 8), :]
            bi = near_blk[1, q, pl.ds(d * 8, 8), :]
            xr = spread_rows[pl.ds(d * 8, 8), pl.ds(q * 128, 128)]
            xi = spread_rows[pl.ds(d * 8, 8), pl.ds(640 + q * 128, 128)]
            sum_re = sum_re + (br * xr - bi * xi)
            sum_im = sum_im + (br * xi + bi * xr)
        image_re.append(sum_re)
        image_im.append(sum_im)
    image = jnp.concatenate(
        [jnp.concatenate(image_re, axis=1), jnp.concatenate(image_im, axis=1)], axis=0
    )
    image = times_table(image, collect[...])
    inside = lanes8 < 24
    rows_now = around[0:8, :]
    right_re = jnp.where(inside, rows_now, 0.0)
    right_im = jnp.where(inside, pltpu.roll(rows_now, 96, 1), 0.0)
    one_re = 2.0 * right_re + image[0:8]
    one_im = 2.0 * right_im + image[8:16]

    ahead = times_table(jnp.concatenate([one_re, one_im], axis=0), spread[:, 0:640])
    image_re, image_im = [], []
    for q in range(5):
        br, bi = own_blk[0, q], own_blk[1, q]
        xr = ahead[0:8, q * 128:(q + 1) * 128]
        xi = ahead[8:16, q * 128:(q + 1) * 128]
        image_re.append(br * xr - bi * xi)
        image_im.append(br * xi + bi * xr)
    image = jnp.concatenate(
        [jnp.concatenate(image_re, axis=1), jnp.concatenate(image_im, axis=1)], axis=0
    )
    image = times_table(image, collect[...])
    fr, fi = one_re[0:1], one_im[0:1]
    sr = 2.0 * fr + jnp.sum(image[0:8], axis=0, keepdims=True)
    si = 2.0 * fi + jnp.sum(image[8:16], axis=0, keepdims=True)
    rr, ri = right_re[0:1], right_im[0:1]
    products = (
        fr * fr + fi * fi,
        sr * sr + si * si,
        fr * sr + fi * si,
        fr * si - fi * sr,
        fr * rr + fi * ri,
        fr * ri - fi * rr,
        sr * rr + si * ri,
        sr * ri - si * rr,
    )
    for i, value in enumerate(products):
        gram_rows[pl.ds(i, 1), :] = value
    plane_rows[pl.ds(0, 1)] = row_sums(gram_rows[...])[0:1].reshape(1, 1, 128)
    plane_copies = [
        remote(plane_rows.at[0], plane_rows.at[slot], plane_send, plane_recv, against(offset))
        for offset, slot in plane.items()
        if slot
    ]
    for copy in plane_copies:
        copy.start()

    left = jnp.concatenate([rr, ri, fr, fi], axis=0)
    turned = jnp.concatenate([-ri, rr, -fi, fr], axis=0)
    guess = jnp.zeros((4, 768), F32)
    for p, rows in ((0, left), (1, turned)):
        high = rows.astype(BF16)
        low = (rows - high.astype(F32)).astype(BF16)
        guess = guess + jnp.dot(high[:, 0:32], mv_parts[p, 0], preferred_element_type=F32)
        guess = guess + jnp.dot(low[:, 0:32], mv_parts[p, 0], preferred_element_type=F32)
        guess = guess + jnp.dot(high[:, 0:32], mv_parts[p, 1], preferred_element_type=F32)
    mid[0] = guess
    mid_copies = [
        remote(mid.at[0], mid.at[1 + d], mid_send.at[d], mid_recv.at[d], against(STEPS[d]))
        for d in range(6)
    ]
    for copy in mid_copies:
        copy.start()
    lanes4 = lax.broadcasted_iota(jnp.int32, (4, 128), 1)
    place4 = lax.rem(lanes4, 32)
    for c in range(6):
        now = guess[:, c * 128:(c + 1) * 128]
        mid[7, :, pl.ds(c * 128, 128)] = jnp.where(
            place4 == 31, pltpu.roll(now, 31, 1), pltpu.roll(now, 127, 1)
        )
        mid[8, :, pl.ds(c * 128, 128)] = jnp.where(
            place4 == 0, pltpu.roll(now, 97, 1), pltpu.roll(now, 1, 1)
        )
    loads[8].wait()

    def middle_step(d, sums):
        sums = list(sums)
        for c in range(6):
            br = mblk[pl.ds(d * 144 + c, 24, stride=6), :]
            bi = mblk[pl.ds((9 + d) * 144 + c, 24, stride=6), :]
            for v in range(2):
                xr = mid[d, pl.ds(2 * v, 1), pl.ds(c * 128, 128)]
                xi = mid[d, pl.ds(2 * v + 1, 1), pl.ds(c * 128, 128)]
                sums[2 * v] = sums[2 * v] + (br * xr - bi * xi)
                sums[2 * v + 1] = sums[2 * v + 1] + (br * xi + bi * xr)
        return tuple(sums)

    sums = tuple(jnp.zeros((24, 128), F32) for _ in range(4))
    sums = middle_step(0, sums)
    sums = lax.fori_loop(7, 9, middle_step, sums)

    count = len(plane)
    every = plane_rows.at[pl.ds(1, count - 1)]
    remote(every, every, plane_send, plane_recv, here).wait_recv()
    together = jnp.sum(plane_rows[...].reshape(count, 128), axis=0, keepdims=True)
    line_rows[pl.ds(0, 1)] = together.reshape(1, 1, 128)
    line_copies = [
        remote(line_rows.at[0], line_rows.at[slot], line_send, line_recv, against(offset))
        for offset, slot in line.items()
        if slot
    ]
    for copy in line_copies:
        copy.start()

    for copy in mid_copies:
        copy.wait_recv()
    sums = lax.fori_loop(1, 7, middle_step, sums)
    rows24 = lax.broadcasted_iota(jnp.int32, (24, 128), 0)
    lanes24 = lax.broadcasted_iota(jnp.int32, (24, 128), 1)
    mine = lax.rem(rows24, 4) == lanes24 // 32
    for i in range(4):
        for c in range(6):
            wide[pl.ds(i * 24 + c * 4, 4), :] = jnp.broadcast_to(
                mid[0, pl.ds(i, 1), pl.ds(c * 128, 128)], (4, 128)
            )
    changes = [
        0.2 * jnp.where(mine, wide[pl.ds(i * 24, 24), :], 0.0) - 0.4 * sums[i] for i in range(4)
    ]
    final[pl.ds(0, 96), :] = times_table(jnp.concatenate(changes, axis=0), square[0:128, :])

    count = len(line)
    every = line_rows.at[pl.ds(1, count - 1)]
    remote(every, every, line_send, line_recv, here).wait_recv()
    totals = jnp.sum(line_rows[...].reshape(count, 128), axis=0, keepdims=True)
    first_norm, second_norm, cross_re, cross_im, ar, ai, br, bi = (
        jnp.broadcast_to(totals[:, i:i + 1], (1, 128)) for i in range(8)
    )
    determinant = first_norm * second_norm - cross_re * cross_re - cross_im * cross_im
    one_r = (second_norm * ar - (cross_re * br - cross_im * bi)) / determinant
    one_i = (second_norm * ai - (cross_re * bi + cross_im * br)) / determinant
    two_r = (first_norm * br - (cross_re * ar + cross_im * ai)) / determinant
    two_i = (first_norm * bi - (cross_re * ai - cross_im * ar)) / determinant
    ur, ui, wr, wi = (final[pl.ds(i * 24, 24), :] for i in range(4))
    update_re = final[96:120, :] + (one_r * ur - one_i * ui) + (two_r * wr - two_i * wi)
    update_im = final[120:144, :] + (one_r * ui + one_i * ur) + (two_r * wi + two_i * wr)
    update_re = update_re.astype(BF16).astype(F32)
    update_im = update_im.astype(BF16).astype(F32)
    for s in range(4):
        for c in range(3):
            vr, vi = fine_vector(0, s, c), fine_vector(1, s, c)
            add_re = jnp.sum(vr * update_re - vi * update_im, axis=0, keepdims=True)
            add_im = jnp.sum(vr * update_im + vi * update_re, axis=0, keepdims=True)
            row = s * 3 + c
            sol_ref[pl.ds(row, 1), :] = second[pl.ds(row, 1), :] + add_re
            sol_ref[pl.ds(12 + row, 1), :] = second[pl.ds(12 + row, 1), :] + add_im

    for copy in first_copies + second_copies + blk_copies + right_copies + mid_copies:
        copy.wait_send()
    every = plane_rows.at[pl.ds(1, len(plane) - 1)]
    remote(every, every, plane_send, plane_recv, here).wait_send()
    every = line_rows.at[pl.ds(1, len(line) - 1)]
    remote(every, every, line_send, line_recv, here).wait_send()


def solution(mesh):
    sizes = tuple(mesh.shape[axis] for axis in ("ta", "gz", "xy"))
    slots = plan(sizes)[1]

    def shards(source_field, gauge_links, fine_vectors, middle_blocks, middle_vectors, bottom_blocks):
        spread, collect, square = (jnp.asarray(t, BF16) for t in tables())
        fine = jnp.transpose(fine_vectors, (0, 1, 3, 4, 5, 6, 2, 7)).reshape(576, 128)
        operands = (
            source_field.reshape(24, 128),
            gauge_links.reshape(144, 128),
            fine,
            middle_blocks.reshape(2592, 128),
            middle_vectors.reshape(288, 128),
            bottom_blocks.reshape(-1, 1, 128),
            spread,
            collect,
            square,
        )
        vmem = [pltpu.VMEM(o.shape, o.dtype) for o in operands]
        dma = pltpu.SemaphoreType.DMA
        sol, res = pl.pallas_call(
            functools.partial(kernel, sizes),
            out_shape=(jax.ShapeDtypeStruct((24, 128), F32),) * 2,
            in_specs=[pl.BlockSpec(memory_space=pltpu.HBM)] * len(operands),
            out_specs=(pl.BlockSpec(memory_space=pltpu.VMEM),) * 2,
            scratch_shapes=vmem
            + [
                pltpu.VMEM((2, 8, 24, 128), F32),
                pltpu.VMEM((24, 128), F32),
                pltpu.VMEM((24, 128), F32),
                pltpu.VMEM((576, 128), F32),
                pltpu.VMEM((2, 2, 32, 768), BF16),
                pltpu.VMEM((2, 5, 8, 128), F32),
                pltpu.VMEM((4, 2, 5, 8, 128), F32),
                pltpu.VMEM((2, 5, 56, 128), F32),
                pltpu.VMEM((len(slots), 1, 128), F32),
                pltpu.VMEM((128, 128), F32),
                pltpu.VMEM((56, 128), F32),
                pltpu.VMEM((56, 1280), F32),
                pltpu.VMEM((128, 128), F32),
                pltpu.VMEM((sizes[0] * sizes[1], 1, 128), F32),
                pltpu.VMEM((sizes[2], 1, 128), F32),
                pltpu.VMEM((9, 4, 768), F32),
                pltpu.VMEM((96, 128), F32),
                pltpu.VMEM((144, 128), F32),
                dma((len(operands),)),
                dma((2, 6)),
                dma((2, 6)),
                dma((4,)),
                dma((4,)),
                dma((len(slots),)),
                dma((len(slots),)),
                dma,
                dma,
                dma,
                dma,
                dma((6,)),
                dma((6,)),
            ],
            compiler_params=pltpu.CompilerParams(collective_id=0, has_side_effects=True),
        )(*operands)
        return sol.reshape(source_field.shape), res.reshape(source_field.shape)

    return jax.shard_map(
        shards,
        mesh=mesh,
        in_specs=(
            P(None, None, None, "ta", "gz", "xy", None),
            P(None, None, None, None, "ta", "gz", "xy", None),
            P(None, None, None, None, "ta", "gz", "xy", None),
            P(None, None, None, "ta", "gz", "xy", None),
            P(None, None, "ta", "gz", "xy", None),
            P(None, None, "ta", "gz", None),
        ),
        out_specs=(
            P(None, None, None, "ta", "gz", "xy", None),
            P(None, None, None, "ta", "gz", "xy", None),
        ),
        check_vma=False,
    )
```

```python
import functools

import jax
import jax.numpy as jnp
import numpy as np
from jax import lax
from jax.experimental import pallas as pl
from jax.experimental.pallas import tpu as pltpu
from jax.sharding import PartitionSpec as P

MESH = pl.DeviceIdType.MESH
F32 = jnp.float32
BF16 = jnp.bfloat16

DIAGONAL = 4.1
TWIST = 0.1
DENOMINATOR = DIAGONAL * DIAGONAL + TWIST * TWIST
PRE_SAME = 0.8 * DIAGONAL / DENOMINATOR
PRE_OTHER = 0.8 * TWIST / DENOMINATOR

STEPS = ((1, 0, 0), (-1, 0, 0), (0, 1, 0), (0, -1, 0), (0, 0, 1), (0, 0, -1))
NEAR = ((0, 0, 0),) + STEPS


def added(one, other):
    return tuple(a + b for a, b in zip(one, other))


def plan(sizes):
    def wrapped(offset):
        return tuple(o % n for o, n in zip(offset, sizes))

    slots = {}
    for one in NEAR:
        for other in NEAR:
            slots.setdefault(wrapped(added(one, other)), len(slots))
    plane = {}
    for dt in range(sizes[0]):
        for dz in range(sizes[1]):
            plane[(dt, dz, 0)] = len(plane)
    line = {(0, 0, dx): dx for dx in range(sizes[2])}
    return wrapped, slots, plane, line


def tables():
    lane = np.arange(128)
    spread = np.zeros((128, 1280), np.float32)
    collect = np.zeros((640, 128), np.float32)
    for j in range(24):
        for k in range(24):
            spread[k, j * 24 + k] = 1
            spread[32 + k, 640 + j * 24 + k] = 1
            collect[j * 24 + k, j] = 1
    unfold = (lane[:, None] % 32 == lane[None] // 4).astype(np.float32)
    share = (lane[:, None] // 4 == lane[None] // 4).astype(np.float32)
    square = np.concatenate([unfold, unfold.T, share], 0)
    return spread, collect, square


def pieces(value):
    high = value.astype(BF16)
    rest = value - high.astype(F32)
    middle = rest.astype(BF16)
    low = (rest - middle.astype(F32)).astype(BF16)
    return high, middle, low


def times_table(value, table):
    high, middle, low = pieces(value)
    return (
        jnp.dot(high, table, preferred_element_type=F32)
        + jnp.dot(middle, table, preferred_element_type=F32)
        + jnp.dot(low, table, preferred_element_type=F32)
    )


def row_sums(value):
    ones = jnp.ones((8, 128), BF16)
    dims = (((1,), (1,)), ((), ()))
    return sum(
        lax.dot_general(ones, piece, dims, preferred_element_type=F32) for piece in pieces(value)
    )


def kernel(
    sizes,
    src_h, gauge_h, fine_h, mblk_h, mvec_h, bblk_h, spread_h, collect_h, square_h,
    sol_ref, res_ref,
    src, gauge, fine, mblk, mvec, bblk, spread, collect, square,
    halo, hop_rows, second, fine_f, mv_parts, own_blk, got_blk, near_blk,
    right_rows, sum_rows, around, spread_rows, gram_rows, plane_rows, line_rows, mid, wide, final,
    local_sem, halo_send, halo_recv, blk_send, blk_recv, right_send, right_recv,
    plane_send, plane_recv, line_send, line_recv, mid_send, mid_recv, near_token, far_token,
):
    wrapped, slots, plane, line = plan(sizes)
    here = tuple(lax.axis_index(axis) for axis in ("ta", "gz", "xy"))

    def at(offset):
        return tuple(
            h if o % n == 0 else lax.rem(h + (o % n), n) for h, o, n in zip(here, offset, sizes)
        )

    def against(offset):
        return at(tuple(-o for o in offset))

    loads = [
        pltpu.make_async_copy(a, b, local_sem.at[i])
        for i, (a, b) in enumerate(
            (
                (src_h, src), (gauge_h, gauge), (bblk_h, bblk), (fine_h, fine), (mvec_h, mvec),
                (spread_h, spread), (collect_h, collect), (square_h, square), (mblk_h, mblk),
            )
        )
    ]
    for load in loads:
        load.start()

    barrier = pltpu.get_barrier_semaphore()
    for step in STEPS:
        pl.semaphore_signal(barrier, inc=1, device_id=at(step), device_id_type=MESH)

    def remote(source, target, send, recv, device):
        return pltpu.make_async_remote_copy(
            src_ref=source, dst_ref=target, send_sem=send, recv_sem=recv,
            device_id=device, device_id_type=MESH,
        )

    class Group:
        def __init__(self, source, target, send, recv, places):
            self.all = [
                remote(source, target.at[slot], send, recv, against(offset)) for offset, slot in places
            ]
            low = min(slot for _, slot in places)
            whole = target.at[pl.ds(low, len(places))]
            self.sum = remote(whole, whole, send, recv, here)

        def start(self):
            for copy in self.all:
                copy.start()
            return self

        def arrived(self):
            self.sum.wait_recv()

        def sent(self):
            self.sum.wait_send()

    def greet(offsets, token):
        far = [offset for offset in offsets if any(wrapped(offset))]
        for offset in far:
            pl.semaphore_signal(token, inc=1, device_id=at(offset), device_id_type=MESH)
        return len(far)

    six = [(STEPS[d], d) for d in range(6)]

    loads[0].wait()
    pl.semaphore_wait(barrier, len(STEPS))
    first_copies = Group(src, halo.at[0], halo_send.at[0], halo_recv.at[0], six).start()

    lanes8 = lax.broadcasted_iota(jnp.int32, (8, 128), 1)
    low_half = lanes8 < 64
    near_blk[...] = jnp.zeros_like(near_blk)
    own_blk[...] = jnp.zeros_like(own_blk)
    around[...] = jnp.zeros_like(around)
    sum_rows[...] = jnp.zeros_like(sum_rows)
    gram_rows[...] = jnp.zeros_like(gram_rows)
    mv_parts[...] = jnp.zeros_like(mv_parts)
    loads[2].wait()
    per_x = bblk.shape[0] // 14

    def site_blocks(x):
        start = (x * 9) // 2
        odd = lax.rem(x, 2) == 1
        for p in range(2):
            chunks = [
                bblk[pl.ds(p * 7 * per_x + start + q, 7, stride=per_x), 0, :] for q in range(5)
            ]
            for q in range(5):
                here_now = chunks[q]
                after = chunks[min(q + 1, 4)]
                moved = jnp.where(
                    low_half[:7], pltpu.roll(here_now, 64, 1), pltpu.roll(after, 64, 1)
                )
                yield p, q, jnp.where(odd, moved, here_now)

    for p, q, value in site_blocks(here[2]):
        own_blk[p, q, pl.ds(0, 7), :] = value
        near_blk[p, q, pl.ds(0, 7, stride=8), :] = value
    for d in (4, 5):
        for p, q, value in site_blocks(at(STEPS[d])[2]):
            near_blk[p, q, pl.ds(1 + d, 7, stride=8), :] = value
    loads[3].wait()
    fine_f[...] = fine[...].astype(F32)
    loads[4].wait()
    for p in range(2):
        for c in range(6):
            block = mvec[pl.ds(p * 144 + c, 24, stride=6), :]
            high = block.astype(BF16)
            mv_parts[p, 0, pl.ds(0, 24), pl.ds(c * 128, 128)] = high
            mv_parts[p, 1, pl.ds(0, 24), pl.ds(c * 128, 128)] = (block - high.astype(F32)).astype(BF16)

    direction = lax.broadcasted_iota(jnp.int32, (8, 128), 0)
    is_t = direction < 2
    is_z = direction < 4
    is_x = direction < 6
    odd_one = lax.rem(direction, 2) == 1
    base = jnp.where(odd_one, 1.0, -1.0).astype(F32)
    in_z = jnp.logical_and(is_z, jnp.logical_not(is_t))
    in_x = jnp.logical_and(is_x, jnp.logical_not(is_z))
    in_y = jnp.logical_not(is_x)

    def flipped(mask):
        return jnp.where(mask, -base, base)

    sign_a = flipped(jnp.logical_not(is_t))
    sign_b = flipped(in_y)
    sign_c = flipped(in_x)
    sign_d = flipped(in_z)
    sign_e = flipped(jnp.logical_or(in_z, in_x))
    sign_f = flipped(jnp.logical_or(in_z, in_y))
    sign_g = flipped(jnp.logical_or(in_x, in_y))

    def pick(a, b, c, d):
        return jnp.where(is_t, a, jnp.where(is_z, b, jnp.where(is_x, c, d)))

    loads[1].wait()

    def hopping(near):
        link = [
            [[gauge[pl.ds(p * 72 + c * 3 + e, 8, stride=9), :] for e in range(3)] for c in range(3)]
            for p in range(2)
        ]
        (r0, r1, r2, r3), (i0, i1, i2, i3) = near
        half = [[[None] * 3 for _ in range(2)] for _ in range(2)]
        for c in range(3):
            half[0][0][c] = r0[c] + sign_a * pick(r2[c], i2[c], i3[c], r3[c])
            half[1][0][c] = i0[c] + sign_b * pick(i2[c], r2[c], r3[c], i3[c])
            half[0][1][c] = r1[c] + sign_c * pick(r3[c], i3[c], i2[c], r2[c])
            half[1][1][c] = i1[c] + sign_d * pick(i3[c], r3[c], r2[c], i2[c])

        def put(p, s, c, value):
            hop_rows[pl.ds(p * 12 + s * 3 + c, 1), :] = jnp.sum(value, axis=0, keepdims=True)

        for c in range(3):
            moved = [[0.0, 0.0], [0.0, 0.0]]
            for s in range(2):
                for e in range(3):
                    lr, li = link[0][c][e], link[1][c][e]
                    hr, hi = half[0][s][e], half[1][s][e]
                    moved[0][s] = moved[0][s] + (lr * hr - li * hi)
                    moved[1][s] = moved[1][s] + (lr * hi + li * hr)
            (a0, a1), (b0, b1) = moved
            put(0, 0, c, a0)
            put(0, 1, c, a1)
            put(1, 0, c, b0)
            put(1, 1, c, b1)
            put(0, 2, c, base * pick(a0, b0, b1, a1))
            put(1, 2, c, sign_e * pick(b0, a0, a1, b1))
            put(0, 3, c, sign_f * pick(a1, b1, b0, a0))
            put(1, 3, c, sign_g * pick(b1, a1, a0, b0))

    def near_values(which):
        return [
            [
                [halo[which, :, p * 12 + s * 3 + c, :] for c in range(3)]
                for s in range(4)
            ]
            for p in range(2)
        ]

    def fill_y(which, field):
        halo[which, 6] = pltpu.roll(field, 127, 1)
        halo[which, 7] = pltpu.roll(field, 1, 1)

    rows12 = lax.broadcasted_iota(jnp.int32, (12, 128), 0)
    chiral = jnp.where(rows12 < 6, 1.0, -1.0).astype(F32)

    def smoothed(re, im):
        return (
            PRE_SAME * re + PRE_OTHER * (chiral * im),
            PRE_SAME * im - PRE_OTHER * (chiral * re),
        )

    def residual(re, im):
        hop_re, hop_im = hop_rows[0:12, :], hop_rows[12:24, :]
        out_re = src[0:12, :] - (DIAGONAL * re - TWIST * (chiral * im) - 0.5 * hop_re)
        out_im = src[12:24, :] - (DIAGONAL * im + TWIST * (chiral * re) - 0.5 * hop_im)
        return out_re, out_im

    fill_y(0, src[...])
    first_copies.arrived()
    near_count = greet([(2, 0, 0), (-2, 0, 0), (0, 0, 2), (0, 0, -2)], near_token)
    raw = near_values(0)
    ready = [[[None] * 3 for _ in range(4)] for _ in range(2)]
    for s in range(4):
        other = PRE_OTHER if s < 2 else -PRE_OTHER
        for c in range(3):
            re, im = raw[0][s][c], raw[1][s][c]
            ready[0][s][c] = PRE_SAME * re + other * im
            ready[1][s][c] = PRE_SAME * im - other * re
    hopping(ready)
    first_re, first_im = smoothed(src[0:12, :], src[12:24, :])
    left_re, left_im = smoothed(*residual(first_re, first_im))
    second_re, second_im = first_re + left_re, first_im + left_im
    second[0:12, :] = second_re
    second[12:24, :] = second_im
    second_copies = Group(second, halo.at[1], halo_send.at[1], halo_recv.at[1], six).start()
    blk_copies = Group(own_blk, got_blk, blk_send, blk_recv, six[:4]).start()
    for load in loads[5:8]:
        load.wait()

    fill_y(1, second[...])
    second_copies.arrived()
    hopping(near_values(1))
    res_re, res_im = residual(second_re, second_im)
    res_ref[0:12, :] = res_re
    res_ref[12:24, :] = res_im
    hop_rows[0:12, :] = res_re.astype(BF16).astype(F32)
    hop_rows[12:24, :] = res_im.astype(BF16).astype(F32)

    def fine_vector(p, s, c):
        return fine_f[pl.ds(p * 288 + c * 4 + s, 24, stride=12), :]

    part_re = jnp.zeros((24, 128), F32)
    part_im = jnp.zeros((24, 128), F32)
    for s in range(4):
        for c in range(3):
            vr, vi = fine_vector(0, s, c), fine_vector(1, s, c)
            rr = hop_rows[pl.ds(s * 3 + c, 1), :]
            ri = hop_rows[pl.ds(12 + s * 3 + c, 1), :]
            part_re = part_re + (vr * rr + vi * ri)
            part_im = part_im + (vr * ri - vi * rr)
    parts = jnp.concatenate([part_re, part_im], axis=0)
    wide[0:48, :] = times_table(parts, square[128:256, :])
    lane_row = lax.broadcasted_iota(jnp.int32, (1, 128), 1)

    def middle_row(p, c):
        rows = [wide[pl.ds(p * 24 + c * 4 + g, 1), :] for g in range(4)]
        return jnp.where(
            lane_row < 64,
            jnp.where(lane_row < 32, rows[0], rows[1]),
            jnp.where(lane_row < 96, rows[2], rows[3]),
        )

    q_re = jnp.zeros((24, 128), F32)
    q_im = jnp.zeros((24, 128), F32)
    for c in range(6):
        vr = mvec[pl.ds(c, 24, stride=6), :]
        vi = mvec[pl.ds(144 + c, 24, stride=6), :]
        mr, mi = middle_row(0, c), middle_row(1, c)
        q_re = q_re + (vr * mr + vi * mi)
        q_im = q_im + (vr * mi - vi * mr)
    sum_rows[0:24, :] = q_re
    sum_rows[32:56, :] = q_im
    right_rows[pl.ds(0, 1)] = row_sums(sum_rows[...])[0:1].reshape(1, 1, 128)

    if near_count:
        pl.semaphore_wait(near_token, near_count)
    right_copies = Group(
        right_rows.at[0], right_rows, right_send, right_recv, [o for o in slots.items() if o[1]]
    ).start()
    final[pl.ds(96, 48), :] = 0.4 * times_table(parts, square[256:384, :])
    blk_copies.arrived()
    for d in range(4):
        for p in range(2):
            for q in range(5):
                near_blk[p, q, pl.ds(1 + d, 7, stride=8), :] = got_blk[d, p, q, pl.ds(0, 7), :]
    right_copies.arrived()
    far_count = greet([(4, 0, 0), (-4, 0, 0)], far_token)

    for d in range(7):
        for i in range(7):
            slot = slots[wrapped(added(NEAR[d], NEAR[i]))]
            around[pl.ds(d * 8 + i, 1), :] = right_rows[slot]
    spread_rows[...] = times_table(around[...], spread[...])
    image_re, image_im = [], []
    for q in range(5):
        sum_re = jnp.zeros((8, 128), F32)
        sum_im = jnp.zeros((8, 128), F32)
        for d in range(7):
            br = near_blk[0, q, pl.ds(d * 8, 8), :]
            bi = near_blk[1, q, pl.ds(d * 8, 8), :]
            xr = spread_rows[pl.ds(d * 8, 8), pl.ds(q * 128, 128)]
            xi = spread_rows[pl.ds(d * 8, 8), pl.ds(640 + q * 128, 128)]
            sum_re = sum_re + (br * xr - bi * xi)
            sum_im = sum_im + (br * xi + bi * xr)
        image_re.append(sum_re)
        image_im.append(sum_im)
    image = jnp.concatenate(
        [jnp.concatenate(image_re, axis=1), jnp.concatenate(image_im, axis=1)], axis=0
    )
    image = times_table(image, collect[...])
    inside = lanes8 < 24
    rows_now = around[0:8, :]
    right_re = jnp.where(inside, rows_now, 0.0)
    right_im = jnp.where(inside, pltpu.roll(rows_now, 96, 1), 0.0)
    one_re = 2.0 * right_re + image[0:8]
    one_im = 2.0 * right_im + image[8:16]

    ahead = times_table(jnp.concatenate([one_re, one_im], axis=0), spread[:, 0:640])
    image_re, image_im = [], []
    for q in range(5):
        br, bi = own_blk[0, q], own_blk[1, q]
        xr = ahead[0:8, q * 128:(q + 1) * 128]
        xi = ahead[8:16, q * 128:(q + 1) * 128]
        image_re.append(br * xr - bi * xi)
        image_im.append(br * xi + bi * xr)
    image = jnp.concatenate(
        [jnp.concatenate(image_re, axis=1), jnp.concatenate(image_im, axis=1)], axis=0
    )
    image = times_table(image, collect[...])
    fr, fi = one_re[0:1], one_im[0:1]
    sr = 2.0 * fr + jnp.sum(image[0:8], axis=0, keepdims=True)
    si = 2.0 * fi + jnp.sum(image[8:16], axis=0, keepdims=True)
    rr, ri = right_re[0:1], right_im[0:1]
    products = (
        fr * fr + fi * fi,
        sr * sr + si * si,
        fr * sr + fi * si,
        fr * si - fi * sr,
        fr * rr + fi * ri,
        fr * ri - fi * rr,
        sr * rr + si * ri,
        sr * ri - si * rr,
    )
    for i, value in enumerate(products):
        gram_rows[pl.ds(i, 1), :] = value
    line_rows[pl.ds(0, 1)] = row_sums(gram_rows[...])[0:1].reshape(1, 1, 128)
    line_copies = Group(
        line_rows.at[0], line_rows, line_send, line_recv, [o for o in line.items() if o[1]]
    ).start()

    left = jnp.concatenate([rr, ri, fr, fi], axis=0)
    turned = jnp.concatenate([-ri, rr, -fi, fr], axis=0)
    guess = jnp.zeros((4, 768), F32)
    for p, rows in ((0, left), (1, turned)):
        high = rows.astype(BF16)
        low = (rows - high.astype(F32)).astype(BF16)
        guess = guess + jnp.dot(high[:, 0:32], mv_parts[p, 0], preferred_element_type=F32)
        guess = guess + jnp.dot(low[:, 0:32], mv_parts[p, 0], preferred_element_type=F32)
        guess = guess + jnp.dot(high[:, 0:32], mv_parts[p, 1], preferred_element_type=F32)
    mid[0] = guess
    mid_copies = Group(
        mid.at[0], mid, mid_send, mid_recv, [(STEPS[d], 1 + d) for d in range(6)]
    ).start()
    lanes4 = lax.broadcasted_iota(jnp.int32, (4, 128), 1)
    place4 = lax.rem(lanes4, 32)
    for c in range(6):
        now = guess[:, c * 128:(c + 1) * 128]
        mid[7, :, pl.ds(c * 128, 128)] = jnp.where(
            place4 == 31, pltpu.roll(now, 31, 1), pltpu.roll(now, 127, 1)
        )
        mid[8, :, pl.ds(c * 128, 128)] = jnp.where(
            place4 == 0, pltpu.roll(now, 97, 1), pltpu.roll(now, 1, 1)
        )
    loads[8].wait()

    def middle_step(d, sums):
        sums = list(sums)
        for c in range(6):
            br = mblk[pl.ds(d * 144 + c, 24, stride=6), :]
            bi = mblk[pl.ds((9 + d) * 144 + c, 24, stride=6), :]
            for v in range(2):
                xr = mid[d, pl.ds(2 * v, 1), pl.ds(c * 128, 128)]
                xi = mid[d, pl.ds(2 * v + 1, 1), pl.ds(c * 128, 128)]
                sums[2 * v] = sums[2 * v] + (br * xr - bi * xi)
                sums[2 * v + 1] = sums[2 * v + 1] + (br * xi + bi * xr)
        return tuple(sums)

    sums = tuple(jnp.zeros((24, 128), F32) for _ in range(4))
    sums = middle_step(0, sums)
    sums = lax.fori_loop(7, 9, middle_step, sums)

    line_copies.arrived()
    together = jnp.sum(line_rows[...].reshape(len(line), 128), axis=0, keepdims=True)
    plane_rows[pl.ds(0, 1)] = together.reshape(1, 1, 128)
    if far_count:
        pl.semaphore_wait(far_token, far_count)
    plane_copies = Group(
        plane_rows.at[0], plane_rows, plane_send, plane_recv, [o for o in plane.items() if o[1]]
    ).start()

    mid_copies.arrived()
    sums = lax.fori_loop(1, 7, middle_step, sums)
    rows24 = lax.broadcasted_iota(jnp.int32, (24, 128), 0)
    lanes24 = lax.broadcasted_iota(jnp.int32, (24, 128), 1)
    mine = lax.rem(rows24, 4) == lanes24 // 32
    for i in range(4):
        for c in range(6):
            wide[pl.ds(i * 24 + c * 4, 4), :] = jnp.broadcast_to(
                mid[0, pl.ds(i, 1), pl.ds(c * 128, 128)], (4, 128)
            )
    changes = [
        0.2 * jnp.where(mine, wide[pl.ds(i * 24, 24), :], 0.0) - 0.4 * sums[i] for i in range(4)
    ]
    final[pl.ds(0, 96), :] = times_table(jnp.concatenate(changes, axis=0), square[0:128, :])

    plane_copies.arrived()
    totals = jnp.sum(plane_rows[...].reshape(len(plane), 128), axis=0, keepdims=True)
    first_norm, second_norm, cross_re, cross_im, ar, ai, br, bi = (
        jnp.broadcast_to(totals[:, i:i + 1], (1, 128)) for i in range(8)
    )
    determinant = first_norm * second_norm - cross_re * cross_re - cross_im * cross_im
    one_r = (second_norm * ar - (cross_re * br - cross_im * bi)) / determinant
    one_i = (second_norm * ai - (cross_re * bi + cross_im * br)) / determinant
    two_r = (first_norm * br - (cross_re * ar + cross_im * ai)) / determinant
    two_i = (first_norm * bi - (cross_re * ai - cross_im * ar)) / determinant
    ur, ui, wr, wi = (final[pl.ds(i * 24, 24), :] for i in range(4))
    update_re = final[96:120, :] + (one_r * ur - one_i * ui) + (two_r * wr - two_i * wi)
    update_im = final[120:144, :] + (one_r * ui + one_i * ur) + (two_r * wi + two_i * wr)
    update_re = update_re.astype(BF16).astype(F32)
    update_im = update_im.astype(BF16).astype(F32)
    for s in range(4):
        for c in range(3):
            vr, vi = fine_vector(0, s, c), fine_vector(1, s, c)
            add_re = jnp.sum(vr * update_re - vi * update_im, axis=0, keepdims=True)
            add_im = jnp.sum(vr * update_im + vi * update_re, axis=0, keepdims=True)
            row = s * 3 + c
            sol_ref[pl.ds(row, 1), :] = second[pl.ds(row, 1), :] + add_re
            sol_ref[pl.ds(12 + row, 1), :] = second[pl.ds(12 + row, 1), :] + add_im

    for group in (
        first_copies, second_copies, blk_copies, right_copies, line_copies, mid_copies, plane_copies
    ):
        group.sent()


def deliver(sol_v, res_v, sol_h, res_h, sem):
    copies = (
        pltpu.make_async_copy(sol_v, sol_h, sem.at[0]),
        pltpu.make_async_copy(res_v, res_h, sem.at[1]),
    )
    for copy in copies:
        copy.start()
    for copy in copies:
        copy.wait()


def solution(mesh):
    sizes = tuple(mesh.shape[axis] for axis in ("ta", "gz", "xy"))
    slots = plan(sizes)[1]

    def shards(source_field, gauge_links, fine_vectors, middle_blocks, middle_vectors, bottom_blocks):
        spread, collect, square = (jnp.asarray(t, BF16) for t in tables())
        fine = jnp.transpose(fine_vectors, (0, 1, 3, 4, 5, 6, 2, 7)).reshape(576, 128)
        operands = (
            source_field.reshape(24, 128),
            gauge_links.reshape(144, 128),
            fine,
            middle_blocks.reshape(2592, 128),
            middle_vectors.reshape(288, 128),
            bottom_blocks.reshape(-1, 1, 128),
            spread,
            collect,
            square,
        )
        vmem = [pltpu.VMEM(o.shape, o.dtype) for o in operands]
        dma = pltpu.SemaphoreType.DMA
        sol, res = pl.pallas_call(
            functools.partial(kernel, sizes),
            out_shape=(pltpu.VMEM((24, 128), F32),) * 2,
            in_specs=[pl.BlockSpec(memory_space=pltpu.HBM)] * len(operands),
            out_specs=(pl.BlockSpec(memory_space=pltpu.VMEM),) * 2,
            scratch_shapes=vmem
            + [
                pltpu.VMEM((2, 8, 24, 128), F32),
                pltpu.VMEM((24, 128), F32),
                pltpu.VMEM((24, 128), F32),
                pltpu.VMEM((576, 128), F32),
                pltpu.VMEM((2, 2, 32, 768), BF16),
                pltpu.VMEM((2, 5, 8, 128), F32),
                pltpu.VMEM((4, 2, 5, 8, 128), F32),
                pltpu.VMEM((2, 5, 56, 128), F32),
                pltpu.VMEM((len(slots), 1, 128), F32),
                pltpu.VMEM((128, 128), F32),
                pltpu.VMEM((56, 128), F32),
                pltpu.VMEM((56, 1280), F32),
                pltpu.VMEM((128, 128), F32),
                pltpu.VMEM((sizes[0] * sizes[1], 1, 128), F32),
                pltpu.VMEM((sizes[2], 1, 128), F32),
                pltpu.VMEM((9, 4, 768), F32),
                pltpu.VMEM((96, 128), F32),
                pltpu.VMEM((144, 128), F32),
                dma((len(operands),)),
                dma((2,)),
                dma((2,)),
            ]
            + [dma] * 10
            + [pltpu.SemaphoreType.REGULAR] * 2,
            compiler_params=pltpu.CompilerParams(collective_id=0, has_side_effects=True),
        )(*operands)
        sol, res = pl.pallas_call(
            deliver,
            out_shape=(jax.ShapeDtypeStruct((24, 128), F32),) * 2,
            in_specs=[pl.BlockSpec(memory_space=pltpu.VMEM)] * 2,
            out_specs=(pl.BlockSpec(memory_space=pltpu.HBM),) * 2,
            scratch_shapes=[pltpu.SemaphoreType.DMA((2,))],
        )(*(pltpu.with_memory_space_constraint(o, pltpu.VMEM) for o in (sol, res)))
        return sol.reshape(source_field.shape), res.reshape(source_field.shape)

    return jax.shard_map(
        shards,
        mesh=mesh,
        in_specs=(
            P(None, None, None, "ta", "gz", "xy", None),
            P(None, None, None, None, "ta", "gz", "xy", None),
            P(None, None, None, None, "ta", "gz", "xy", None),
            P(None, None, None, "ta", "gz", "xy", None),
            P(None, None, "ta", "gz", "xy", None),
            P(None, None, "ta", "gz", None),
        ),
        out_specs=(
            P(None, None, None, "ta", "gz", "xy", None),
            P(None, None, None, "ta", "gz", "xy", None),
        ),
        check_vma=False,
    )
```

```python
import functools

import jax
import jax.numpy as jnp
from jax import lax
from jax.experimental import pallas as pl
from jax.experimental.pallas import tpu as pltpu
from jax.sharding import PartitionSpec as P

MESH = pl.DeviceIdType.MESH
F32 = jnp.float32
BF16 = jnp.bfloat16

DIAGONAL = 4.1
TWIST = 0.1
DENOMINATOR = DIAGONAL * DIAGONAL + TWIST * TWIST
PRE_SAME = 0.8 * DIAGONAL / DENOMINATOR
PRE_OTHER = 0.8 * TWIST / DENOMINATOR

STEPS = ((1, 0, 0), (-1, 0, 0), (0, 1, 0), (0, -1, 0), (0, 0, 1), (0, 0, -1))
NEAR = ((0, 0, 0),) + STEPS


def added(one, other):
    return tuple(a + b for a, b in zip(one, other))


def plan(sizes):
    def wrapped(offset):
        return tuple(o % n for o, n in zip(offset, sizes))

    slots = {}
    for one in NEAR:
        for other in NEAR:
            slots.setdefault(wrapped(added(one, other)), len(slots))
    plane = {}
    for dt in range(sizes[0]):
        for dz in range(sizes[1]):
            plane[(dt, dz, 0)] = len(plane)
    line = {(0, 0, dx): dx for dx in range(sizes[2])}
    return wrapped, slots, plane, line


def pieces(value):
    high = value.astype(BF16)
    rest = value - high.astype(F32)
    middle = rest.astype(BF16)
    low = (rest - middle.astype(F32)).astype(BF16)
    return high, middle, low


def row_sums(value):
    ones = jnp.ones((8, 384), BF16)
    dims = (((1,), (1,)), ((), ()))
    stacked = jnp.concatenate(pieces(value), axis=1)
    return lax.dot_general(ones, stacked, dims, preferred_element_type=F32)


def lanes_from(value, places):
    return jnp.take_along_axis(
        value, jnp.broadcast_to(places, value.shape), axis=1, mode="promise_in_bounds"
    )


def four_groups(value):
    return (value + pltpu.roll(value, 32, 1)) + (pltpu.roll(value, 64, 1) + pltpu.roll(value, 96, 1))


def four_lanes(value, first):
    one, two, three, four = (lanes_from(value, first + b) for b in range(4))
    return (one + two) + (three + four)


def distance(offset, sizes):
    t, z, x = (min(o % n, n - o % n) for o, n in zip(offset, sizes))
    return t / 2 + (t % 2) / 2 + z + x


def kernel(
    sizes,
    src_h, gauge_h, fine_h, mblk_h, mvec_h, bblk_h,
    sol_ref, res_ref,
    src, gauge, fine, mblk, mvec, bblk,
    halo, half_out, hop_rows, first, second, fine_f, mv_parts, own_blk, got_blk, near_blk,
    right_rows, sum_rows, around, plane_rows, line_rows, mid, wide, final,
    local_sem, halo_send, halo_recv, blk_send, blk_recv, right_send, right_recv,
    plane_send, plane_recv, line_send, line_recv, mid_send, mid_recv, mid_line_send, mid_line_recv,
    near_token, far_token,
):
    wrapped, slots, plane, line = plan(sizes)
    here = tuple(lax.axis_index(axis) for axis in ("ta", "gz", "xy"))

    def at(offset):
        return tuple(
            h if o % n == 0 else lax.rem(h + (o % n), n) for h, o, n in zip(here, offset, sizes)
        )

    def against(offset):
        return at(tuple(-o for o in offset))

    loads = [
        pltpu.make_async_copy(a, b, local_sem.at[i])
        for i, (a, b) in enumerate(
            (
                (src_h, src), (gauge_h, gauge), (bblk_h, bblk), (fine_h, fine), (mvec_h, mvec),
                (mblk_h, mblk),
            )
        )
    ]
    for load in loads:
        load.start()

    barrier = pltpu.get_barrier_semaphore()
    for step in STEPS:
        pl.semaphore_signal(barrier, inc=1, device_id=at(step), device_id_type=MESH)

    def remote(source, target, send, recv, device):
        return pltpu.make_async_remote_copy(
            src_ref=source, dst_ref=target, send_sem=send, recv_sem=recv,
            device_id=device, device_id_type=MESH,
        )

    class Group:
        def __init__(self, source, target, send, recv, places):
            places = sorted(places, key=lambda place: -distance(place[0], sizes))
            self.all = [
                remote(
                    source(slot) if callable(source) else source, target.at[pl.ds(slot, 1)],
                    send, recv, against(offset),
                )
                for offset, slot in places
            ]
            low = min(slot for _, slot in places)
            whole = target.at[pl.ds(low, len(places))]
            self.sum = remote(whole, whole, send, recv, here)

        def start(self):
            for copy in self.all:
                copy.start()
            return self

        def arrived(self):
            self.sum.wait_recv()

        def sent(self):
            self.sum.wait_send()

    def greet(offsets, token):
        far = [offset for offset in offsets if any(wrapped(offset))]
        for offset in far:
            pl.semaphore_signal(token, inc=1, device_id=at(offset), device_id_type=MESH)
        return len(far)

    six = [(STEPS[d], d) for d in range(6)]

    rows12 = lax.broadcasted_iota(jnp.int32, (12, 128), 0)
    chiral = jnp.where(rows12 < 6, 1.0, -1.0).astype(F32)

    def smoothed(re, im):
        return (
            PRE_SAME * re + PRE_OTHER * (chiral * im),
            PRE_SAME * im - PRE_OTHER * (chiral * re),
        )

    def send_halves(which, field):
        r0, r1, r2, r3 = (field[pl.ds(s * 3, 3), :] for s in range(4))
        i0, i1, i2, i3 = (field[pl.ds(12 + s * 3, 3), :] for s in range(4))
        for axis, lower in enumerate(
            (
                (r2, r3, i2, i3),
                (-i2, i3, r2, -r3),
                (-i3, -i2, r3, r2),
                (-r3, r2, -i3, i2),
            )
        ):
            for d in (2 * axis, 2 * axis + 1):
                for row, (up, low) in enumerate(zip((r0, r1, i0, i1), lower)):
                    value = up - low if d % 2 == 0 else up + low
                    if axis < 3:
                        half_out[which, d, pl.ds(row * 3, 3), :] = value
                    else:
                        shift = 127 if d == 6 else 1
                        halo[which, d, pl.ds(row * 3, 3), :] = pltpu.roll(value, shift, 1)

    loads[0].wait()
    first_re, first_im = smoothed(src[0:12, :], src[12:24, :])
    first[0:12, :] = first_re
    first[12:24, :] = first_im
    send_halves(0, first)
    pl.semaphore_wait(barrier, len(STEPS))
    first_copies = Group(
        lambda d: half_out.at[0, pl.ds(d, 1)], halo.at[0], halo_send.at[0], halo_recv.at[0], six
    ).start()

    lanes8 = lax.broadcasted_iota(jnp.int32, (8, 128), 1)
    lane_row = lax.broadcasted_iota(jnp.int32, (1, 128), 1)
    near_blk[...] = jnp.zeros_like(near_blk)
    own_blk[...] = jnp.zeros_like(own_blk)
    around[...] = jnp.zeros_like(around)
    sum_rows[...] = jnp.zeros_like(sum_rows)
    right_rows[pl.ds(0, 1), :] = jnp.zeros((1, 128), F32)
    mv_parts[...] = jnp.zeros_like(mv_parts)
    loads[2].wait()
    per_x = bblk.shape[0] // 14

    def site_blocks(x):
        start = (x * 9) // 2
        skipped = lax.rem(x, 2) * 64
        rows = [
            [bblk[pl.ds(p * 7 * per_x + start + q, 7, stride=per_x), 0, :] for q in range(5)]
            for p in range(2)
        ]
        lane = lax.broadcasted_iota(jnp.int32, (7, 128), 1)
        for c in range(6):
            place = lax.rem(lane, 32) * 24 + 4 * c + lane // 32 + skipped
            chunk = place // 128
            within = lax.rem(place, 128)
            valid = lax.rem(lane, 32) < 24
            for p in range(2):
                value = jnp.zeros((7, 128), F32)
                for q in range(5):
                    value = jnp.where(chunk == q, lanes_from(rows[p][q], within), value)
                yield p, c, jnp.where(valid, value, 0.0)

    for p, q, value in site_blocks(here[2]):
        own_blk[0, p, q, pl.ds(0, 7), :] = value
        near_blk[p, q, pl.ds(0, 7, stride=8), :] = value
    for d in (4, 5):
        for p, q, value in site_blocks(at(STEPS[d])[2]):
            near_blk[p, q, pl.ds(1 + d, 7, stride=8), :] = value
    loads[3].wait()
    fine_f[...] = fine[...].astype(F32)
    loads[4].wait()
    for p in range(2):
        for c in range(6):
            block = mvec[pl.ds(p * 144 + c, 24, stride=6), :]
            high = block.astype(BF16)
            mv_parts[p, 0, pl.ds(0, 24), pl.ds(c * 128, 128)] = high
            mv_parts[p, 1, pl.ds(0, 24), pl.ds(c * 128, 128)] = (block - high.astype(F32)).astype(BF16)

    direction = lax.broadcasted_iota(jnp.int32, (8, 128), 0)
    is_t = direction < 2
    is_z = direction < 4
    is_x = direction < 6
    odd_one = lax.rem(direction, 2) == 1
    base = jnp.where(odd_one, 1.0, -1.0).astype(F32)
    in_z = jnp.logical_and(is_z, jnp.logical_not(is_t))
    in_x = jnp.logical_and(is_x, jnp.logical_not(is_z))
    in_y = jnp.logical_not(is_x)

    def flipped(mask):
        return jnp.where(mask, -base, base)

    sign_e = flipped(jnp.logical_or(in_z, in_x))
    sign_f = flipped(jnp.logical_or(in_z, in_y))
    sign_g = flipped(jnp.logical_or(in_x, in_y))

    def pick(a, b, c, d):
        return jnp.where(is_t, a, jnp.where(is_z, b, jnp.where(is_x, c, d)))

    loads[1].wait()

    def hopping(which):
        link = [
            [[gauge[pl.ds(p * 72 + c * 3 + e, 8, stride=9), :] for e in range(3)] for c in range(3)]
            for p in range(2)
        ]
        half = [
            [[halo[which, :, p * 6 + s * 3 + c, :] for c in range(3)] for s in range(2)]
            for p in range(2)
        ]

        def put(p, s, c, value):
            hop_rows[pl.ds(p * 12 + s * 3 + c, 1), :] = jnp.sum(value, axis=0, keepdims=True)

        for c in range(3):
            moved = [[0.0, 0.0], [0.0, 0.0]]
            for s in range(2):
                for e in range(3):
                    lr, li = link[0][c][e], link[1][c][e]
                    hr, hi = half[0][s][e], half[1][s][e]
                    moved[0][s] = moved[0][s] + (lr * hr - li * hi)
                    moved[1][s] = moved[1][s] + (lr * hi + li * hr)
            (a0, a1), (b0, b1) = moved
            put(0, 0, c, a0)
            put(0, 1, c, a1)
            put(1, 0, c, b0)
            put(1, 1, c, b1)
            put(0, 2, c, base * pick(a0, b0, b1, a1))
            put(1, 2, c, sign_e * pick(b0, a0, a1, b1))
            put(0, 3, c, sign_f * pick(a1, b1, b0, a0))
            put(1, 3, c, sign_g * pick(b1, a1, a0, b0))

    def residual(re, im):
        hop_re, hop_im = hop_rows[0:12, :], hop_rows[12:24, :]
        out_re = src[0:12, :] - (DIAGONAL * re - TWIST * (chiral * im) - 0.5 * hop_re)
        out_im = src[12:24, :] - (DIAGONAL * im + TWIST * (chiral * re) - 0.5 * hop_im)
        return out_re, out_im

    first_copies.arrived()
    near_count = greet([(2, 0, 0), (-2, 0, 0), (0, 0, 2), (0, 0, -2)], near_token)
    hopping(0)
    left_re, left_im = smoothed(*residual(first_re, first_im))
    second_re, second_im = first_re + left_re, first_im + left_im
    second[0:12, :] = second_re
    second[12:24, :] = second_im
    send_halves(1, second)
    second_copies = Group(
        lambda d: half_out.at[1, pl.ds(d, 1)], halo.at[1], halo_send.at[1], halo_recv.at[1], six
    ).start()
    blk_copies = Group(own_blk, got_blk, blk_send, blk_recv, six[:4]).start()

    second_copies.arrived()
    hopping(1)
    res_re, res_im = residual(second_re, second_im)
    res_ref[0:12, :] = res_re
    res_ref[12:24, :] = res_im
    hop_rows[0:12, :] = res_re.astype(BF16).astype(F32)
    hop_rows[12:24, :] = res_im.astype(BF16).astype(F32)

    def fine_vector(p, s, c):
        return fine_f[pl.ds(p * 288 + c * 4 + s, 24, stride=12), :]

    part_re = jnp.zeros((24, 128), F32)
    part_im = jnp.zeros((24, 128), F32)
    for s in range(4):
        for c in range(3):
            vr, vi = fine_vector(0, s, c), fine_vector(1, s, c)
            rr = hop_rows[pl.ds(s * 3 + c, 1), :]
            ri = hop_rows[pl.ds(12 + s * 3 + c, 1), :]
            part_re = part_re + (vr * rr + vi * ri)
            part_im = part_im + (vr * ri - vi * rr)
    parts = jnp.concatenate([part_re, part_im], axis=0)
    wide[0:48, :] = four_lanes(parts, 4 * lax.rem(lane_row, 32))

    def middle_row(p, c):
        rows = [wide[pl.ds(p * 24 + c * 4 + g, 1), :] for g in range(4)]
        return jnp.where(
            lane_row < 64,
            jnp.where(lane_row < 32, rows[0], rows[1]),
            jnp.where(lane_row < 96, rows[2], rows[3]),
        )

    q_re = jnp.zeros((24, 128), F32)
    q_im = jnp.zeros((24, 128), F32)
    for c in range(6):
        vr = mvec[pl.ds(c, 24, stride=6), :]
        vi = mvec[pl.ds(144 + c, 24, stride=6), :]
        mr, mi = middle_row(0, c), middle_row(1, c)
        q_re = q_re + (vr * mr + vi * mi)
        q_im = q_im + (vr * mi - vi * mr)
    sum_rows[0:24, :] = q_re
    sum_rows[32:56, :] = q_im
    right_rows[pl.ds(0, 1), pl.ds(0, 64)] = row_sums(sum_rows[...])[0:1]

    if near_count:
        pl.semaphore_wait(near_token, near_count)
    right_copies = Group(
        right_rows.at[pl.ds(0, 1)], right_rows, right_send, right_recv, [o for o in slots.items() if o[1]]
    ).start()
    final[pl.ds(96, 48), :] = 0.4 * four_lanes(parts, 4 * (lane_row // 4))
    blk_copies.arrived()
    for d in range(4):
        for p in range(2):
            for q in range(6):
                near_blk[p, q, pl.ds(1 + d, 7, stride=8), :] = got_blk[d, p, q, pl.ds(0, 7), :]
    right_copies.arrived()
    far_count = greet([(4, 0, 0), (-4, 0, 0)], far_token)

    for d in range(7):
        for i in range(7):
            slot = slots[wrapped(added(NEAR[d], NEAR[i]))]
            around[pl.ds(d * 8 + i, 1), :] = right_rows[pl.ds(slot, 1), :]
    rows_now = around[...]
    sum_re = jnp.zeros((8, 128), F32)
    sum_im = jnp.zeros((8, 128), F32)
    for c in range(6):
        xr = lanes_from(rows_now, 4 * c + lane_row // 32)
        xi = lanes_from(rows_now, 32 + 4 * c + lane_row // 32)
        br, bi = near_blk[0, c], near_blk[1, c]
        term_re = br * xr - bi * xi
        term_im = br * xi + bi * xr
        for d in range(7):
            sum_re = sum_re + term_re[d * 8:(d + 1) * 8]
            sum_im = sum_im + term_im[d * 8:(d + 1) * 8]
    right_re = lanes_from(rows_now[0:8], lax.rem(lane_row, 32))
    right_im = lanes_from(rows_now[0:8], 32 + lax.rem(lane_row, 32))
    one_re = 2.0 * right_re + four_groups(sum_re)
    one_im = 2.0 * right_im + four_groups(sum_im)

    sum_re = jnp.zeros((8, 128), F32)
    sum_im = jnp.zeros((8, 128), F32)
    for c in range(6):
        xr = lanes_from(one_re, 4 * c + lane_row // 32)
        xi = lanes_from(one_im, 4 * c + lane_row // 32)
        br, bi = own_blk[0, 0, c], own_blk[0, 1, c]
        sum_re = sum_re + (br * xr - bi * xi)
        sum_im = sum_im + (br * xi + bi * xr)
    two = four_groups(
        jnp.concatenate(
            [jnp.sum(sum_re, axis=0, keepdims=True), jnp.sum(sum_im, axis=0, keepdims=True)], axis=0
        )
    )
    fr, fi = one_re[0:1], one_im[0:1]
    sr = 2.0 * fr + two[0:1]
    si = 2.0 * fi + two[1:2]
    rr, ri = right_re[0:1], right_im[0:1]
    products = (
        fr * fr + fi * fi,
        sr * sr + si * si,
        fr * sr + fi * si,
        fr * si - fi * sr,
        fr * rr + fi * ri,
        fr * ri - fi * rr,
        sr * rr + si * ri,
        sr * ri - si * rr,
    )
    folded = jnp.concatenate(products, axis=0)
    folded = folded + pltpu.roll(folded, 16, 1)
    rows8 = lax.broadcasted_iota(jnp.int32, (8, 128), 0)
    folded = jnp.where(lanes8 // 16 == rows8, folded, 0.0)
    line_rows[pl.ds(0, 1), :] = jnp.sum(folded, axis=0, keepdims=True)
    line_copies = Group(
        line_rows.at[pl.ds(0, 1)], line_rows, line_send, line_recv, [o for o in line.items() if o[1]]
    ).start()

    left = jnp.concatenate([rr, ri, fr, fi], axis=0)
    turned = jnp.concatenate([-ri, rr, -fi, fr], axis=0)
    guess = jnp.zeros((4, 768), F32)
    for p, rows in ((0, left), (1, turned)):
        high = rows.astype(BF16)
        low = (rows - high.astype(F32)).astype(BF16)
        guess = guess + jnp.dot(high[:, 0:32], mv_parts[p, 0], preferred_element_type=F32)
        guess = guess + jnp.dot(low[:, 0:32], mv_parts[p, 0], preferred_element_type=F32)
        guess = guess + jnp.dot(high[:, 0:32], mv_parts[p, 1], preferred_element_type=F32)
    mid[0] = guess
    mid_copies = Group(
        mid.at[pl.ds(0, 1)], mid, mid_send, mid_recv, [(STEPS[d], 1 + d) for d in range(4)]
    ).start()
    lanes4 = lax.broadcasted_iota(jnp.int32, (4, 128), 1)
    place4 = lax.rem(lanes4, 32)
    for c in range(6):
        now = guess[:, c * 128:(c + 1) * 128]
        mid[7, :, pl.ds(c * 128, 128)] = jnp.where(
            place4 == 31, pltpu.roll(now, 31, 1), pltpu.roll(now, 127, 1)
        )
        mid[8, :, pl.ds(c * 128, 128)] = jnp.where(
            place4 == 0, pltpu.roll(now, 97, 1), pltpu.roll(now, 1, 1)
        )
    loads[5].wait()

    def middle_step(d, sums):
        sums = list(sums)
        for c in range(6):
            br = mblk[pl.ds(d * 144 + c, 24, stride=6), :]
            bi = mblk[pl.ds((9 + d) * 144 + c, 24, stride=6), :]
            for v in range(2):
                xr = mid[d, pl.ds(2 * v, 1), pl.ds(c * 128, 128)]
                xi = mid[d, pl.ds(2 * v + 1, 1), pl.ds(c * 128, 128)]
                sums[2 * v] = sums[2 * v] + (br * xr - bi * xi)
                sums[2 * v + 1] = sums[2 * v + 1] + (br * xi + bi * xr)
        return tuple(sums)

    sums = tuple(jnp.zeros((24, 128), F32) for _ in range(4))
    sums = middle_step(0, sums)
    sums = lax.fori_loop(7, 9, middle_step, sums)

    line_copies.arrived()
    plane_rows[pl.ds(0, 1), :] = jnp.sum(line_rows[...], axis=0, keepdims=True)
    if far_count:
        pl.semaphore_wait(far_token, far_count)
    plane_copies = Group(
        plane_rows.at[pl.ds(0, 1)], plane_rows, plane_send, plane_recv, [o for o in plane.items() if o[1]]
    ).start()

    mid_line_copies = Group(
        mid.at[pl.ds(0, 1)], mid, mid_line_send, mid_line_recv,
        [(STEPS[d], 1 + d) for d in (4, 5)],
    ).start()
    mid_copies.arrived()
    sums = lax.fori_loop(1, 5, middle_step, sums)
    mid_line_copies.arrived()
    sums = lax.fori_loop(5, 7, middle_step, sums)
    rows24 = lax.broadcasted_iota(jnp.int32, (24, 128), 0)
    lanes24 = lax.broadcasted_iota(jnp.int32, (24, 128), 1)
    mine = lax.rem(rows24, 4) == lanes24 // 32
    for i in range(4):
        for c in range(6):
            wide[pl.ds(i * 24 + c * 4, 4), :] = jnp.broadcast_to(
                mid[0, pl.ds(i, 1), pl.ds(c * 128, 128)], (4, 128)
            )
    changes = [
        0.2 * jnp.where(mine, wide[pl.ds(i * 24, 24), :], 0.0) - 0.4 * sums[i] for i in range(4)
    ]
    final[pl.ds(0, 96), :] = lanes_from(
        four_groups(jnp.concatenate(changes, axis=0)), lane_row // 4
    )

    plane_copies.arrived()
    totals = jnp.broadcast_to(jnp.sum(plane_rows[...], axis=0, keepdims=True), (8, 128))
    totals = jnp.sum(jnp.where(lanes8 // 16 == rows8, totals, 0.0), axis=1, keepdims=True)
    first_norm, second_norm, cross_re, cross_im, ar, ai, br, bi = (
        jnp.broadcast_to(totals[i:i + 1, :], (1, 128)) for i in range(8)
    )
    determinant = first_norm * second_norm - cross_re * cross_re - cross_im * cross_im
    one_r = (second_norm * ar - (cross_re * br - cross_im * bi)) / determinant
    one_i = (second_norm * ai - (cross_re * bi + cross_im * br)) / determinant
    two_r = (first_norm * br - (cross_re * ar + cross_im * ai)) / determinant
    two_i = (first_norm * bi - (cross_re * ai - cross_im * ar)) / determinant
    ur, ui, wr, wi = (final[pl.ds(i * 24, 24), :] for i in range(4))
    update_re = final[96:120, :] + (one_r * ur - one_i * ui) + (two_r * wr - two_i * wi)
    update_im = final[120:144, :] + (one_r * ui + one_i * ur) + (two_r * wi + two_i * wr)
    update_re = update_re.astype(BF16).astype(F32)
    update_im = update_im.astype(BF16).astype(F32)
    for s in range(4):
        for c in range(3):
            vr, vi = fine_vector(0, s, c), fine_vector(1, s, c)
            add_re = jnp.sum(vr * update_re - vi * update_im, axis=0, keepdims=True)
            add_im = jnp.sum(vr * update_im + vi * update_re, axis=0, keepdims=True)
            row = s * 3 + c
            sol_ref[pl.ds(row, 1), :] = second[pl.ds(row, 1), :] + add_re
            sol_ref[pl.ds(12 + row, 1), :] = second[pl.ds(12 + row, 1), :] + add_im

    for group in (
        first_copies, second_copies, blk_copies, right_copies, line_copies, mid_copies, plane_copies,
        mid_line_copies,
    ):
        group.sent()


def deliver(sol_v, res_v, sol_h, res_h, sem):
    copies = (
        pltpu.make_async_copy(sol_v, sol_h, sem.at[0]),
        pltpu.make_async_copy(res_v, res_h, sem.at[1]),
    )
    for copy in copies:
        copy.start()
    for copy in copies:
        copy.wait()


def solution(mesh):
    sizes = tuple(mesh.shape[axis] for axis in ("ta", "gz", "xy"))
    slots = plan(sizes)[1]

    def shards(source_field, gauge_links, fine_vectors, middle_blocks, middle_vectors, bottom_blocks):
        fine = jnp.transpose(fine_vectors, (0, 1, 3, 4, 5, 6, 2, 7)).reshape(576, 128)
        operands = (
            source_field.reshape(24, 128),
            gauge_links.reshape(144, 128),
            fine,
            middle_blocks.reshape(2592, 128),
            middle_vectors.reshape(288, 128),
            bottom_blocks.reshape(-1, 1, 128),
        )
        vmem = [pltpu.VMEM(o.shape, o.dtype) for o in operands]
        dma = pltpu.SemaphoreType.DMA
        sol, res = pl.pallas_call(
            functools.partial(kernel, sizes),
            out_shape=(pltpu.VMEM((24, 128), F32),) * 2,
            in_specs=[pl.BlockSpec(memory_space=pltpu.HBM)] * len(operands),
            out_specs=(pl.BlockSpec(memory_space=pltpu.VMEM),) * 2,
            scratch_shapes=vmem
            + [
                pltpu.VMEM((2, 8, 12, 128), F32),
                pltpu.VMEM((2, 6, 12, 128), F32),
                pltpu.VMEM((24, 128), F32),
                pltpu.VMEM((24, 128), F32),
                pltpu.VMEM((24, 128), F32),
                pltpu.VMEM((576, 128), F32),
                pltpu.VMEM((2, 2, 32, 768), BF16),
                pltpu.VMEM((1, 2, 6, 8, 128), F32),
                pltpu.VMEM((4, 2, 6, 8, 128), F32),
                pltpu.VMEM((2, 6, 56, 128), F32),
                pltpu.VMEM((len(slots), 128), F32),
                pltpu.VMEM((64, 128), F32),
                pltpu.VMEM((56, 128), F32),
                pltpu.VMEM((sizes[0] * sizes[1], 128), F32),
                pltpu.VMEM((sizes[2], 128), F32),
                pltpu.VMEM((9, 4, 768), F32),
                pltpu.VMEM((96, 128), F32),
                pltpu.VMEM((144, 128), F32),
                dma((len(operands),)),
                dma((2,)),
                dma((2,)),
            ]
            + [dma] * 12
            + [pltpu.SemaphoreType.REGULAR] * 2,
            compiler_params=pltpu.CompilerParams(collective_id=0, has_side_effects=True),
        )(*operands)
        sol, res = pl.pallas_call(
            deliver,
            out_shape=(jax.ShapeDtypeStruct((24, 128), F32),) * 2,
            in_specs=[pl.BlockSpec(memory_space=pltpu.VMEM)] * 2,
            out_specs=(pl.BlockSpec(memory_space=pltpu.HBM),) * 2,
            scratch_shapes=[pltpu.SemaphoreType.DMA((2,))],
        )(*(pltpu.with_memory_space_constraint(o, pltpu.VMEM) for o in (sol, res)))
        return sol.reshape(source_field.shape), res.reshape(source_field.shape)

    return jax.shard_map(
        shards,
        mesh=mesh,
        in_specs=(
            P(None, None, None, "ta", "gz", "xy", None),
            P(None, None, None, None, "ta", "gz", "xy", None),
            P(None, None, None, None, "ta", "gz", "xy", None),
            P(None, None, None, "ta", "gz", "xy", None),
            P(None, None, "ta", "gz", "xy", None),
            P(None, None, "ta", "gz", None),
        ),
        out_specs=(
            P(None, None, None, "ta", "gz", "xy", None),
            P(None, None, None, "ta", "gz", "xy", None),
        ),
        check_vma=False,
    )
```

```python
import functools

import jax
import jax.numpy as jnp
from jax import lax
from jax.experimental import pallas as pl
from jax.experimental.pallas import tpu as pltpu
from jax.sharding import PartitionSpec as P

MESH = pl.DeviceIdType.MESH
F32 = jnp.float32
BF16 = jnp.bfloat16

DIAGONAL = 4.1
TWIST = 0.1
DENOMINATOR = DIAGONAL * DIAGONAL + TWIST * TWIST
PRE_SAME = 0.8 * DIAGONAL / DENOMINATOR
PRE_OTHER = 0.8 * TWIST / DENOMINATOR

STEPS = ((1, 0, 0), (-1, 0, 0), (0, 1, 0), (0, -1, 0), (0, 0, 1), (0, 0, -1))
NEAR = ((0, 0, 0),) + STEPS
TARGETS = ((0, 1, 0), (2, 0, 0), (2, 1, 0))


def added(one, other):
    return tuple(a + b for a, b in zip(one, other))


def plan(sizes):
    def wrapped(offset):
        return tuple(o % n for o, n in zip(offset, sizes))

    slots = {}
    for one in NEAR:
        for other in NEAR:
            slots.setdefault(wrapped(added(one, other)), len(slots))
    plane = {}
    for dt in range(sizes[0]):
        for dz in range(sizes[1]):
            plane[(dt, dz, 0)] = len(plane)
    line = {(0, 0, dx): dx for dx in range(sizes[2])}
    return wrapped, slots, plane, line


def pieces(value):
    high = value.astype(BF16)
    rest = value - high.astype(F32)
    middle = rest.astype(BF16)
    low = (rest - middle.astype(F32)).astype(BF16)
    return high, middle, low


def row_sums(value):
    ones = jnp.ones((8, 384), BF16)
    dims = (((1,), (1,)), ((), ()))
    stacked = jnp.concatenate(pieces(value), axis=1)
    return lax.dot_general(ones, stacked, dims, preferred_element_type=F32)


def lanes_from(value, places):
    return jnp.take_along_axis(
        value, jnp.broadcast_to(places, value.shape), axis=1, mode="promise_in_bounds"
    )


def four_groups(value):
    return (value + pltpu.roll(value, 32, 1)) + (pltpu.roll(value, 64, 1) + pltpu.roll(value, 96, 1))


def four_lanes(value, first):
    one, two, three, four = (lanes_from(value, first + b) for b in range(4))
    return (one + two) + (three + four)


def distance(offset, sizes):
    t, z, x = (min(o % n, n - o % n) for o, n in zip(offset, sizes))
    return t / 2 + (t % 2) / 2 + z + x


def kernel(
    sizes,
    src_h, gauge_h, fine_h, mblk_h, mvec_h, bblk_h,
    sol_ref, res_ref,
    src, gauge, fine, mblk, mvec, bblk,
    halo, half_out, hop_rows, first, second, fine_f, mv_parts, own_blk, got_blk, near_blk,
    right_rows, sum_rows, around, plane_rows, line_rows, mid, wide, final,
    local_sem, halo_send, halo_recv, blk_send, blk_recv, right_send, right_recv,
    plane_send, plane_recv, line_send, line_recv, mid_send, mid_recv, mid_line_send, mid_line_recv,
    near_token, far_token, all_rows, total_row, all_send, all_recv,
):
    wrapped, slots, plane, line = plan(sizes)
    here = tuple(lax.axis_index(axis) for axis in ("ta", "gz", "xy"))

    def at(offset):
        return tuple(
            h if o % n == 0 else lax.rem(h + (o % n), n) for h, o, n in zip(here, offset, sizes)
        )

    def against(offset):
        return at(tuple(-o for o in offset))

    loads = [
        pltpu.make_async_copy(a, b, local_sem.at[i])
        for i, (a, b) in enumerate(
            (
                (src_h, src), (gauge_h, gauge), (bblk_h, bblk), (fine_h, fine), (mvec_h, mvec),
                (mblk_h, mblk),
            )
        )
    ]
    for load in loads:
        load.start()

    barrier = pltpu.get_barrier_semaphore()
    for step in STEPS:
        pl.semaphore_signal(barrier, inc=1, device_id=at(step), device_id_type=MESH)

    def is_here(place):
        same = [h == o for h, o in zip(here, place)]
        return jnp.logical_and(jnp.logical_and(same[0], same[1]), same[2])

    targets = [t for t in TARGETS if all(o < n for o, n in zip(t, sizes))]
    chosen = [is_here(t) for t in targets]
    served = functools.reduce(jnp.logical_or, chosen)
    squares = sizes[0] * sizes[1]
    for target, mine in zip(targets, chosen):

        @pl.when(mine)
        def _(target=target):
            def greet_square(i, _):
                square = lax.rem(i + squares // 2, squares)
                place = lax.rem(target[0] + square // sizes[1], sizes[0])
                other = lax.rem(target[1] + lax.rem(square, sizes[1]), sizes[1])
                for dx in range(sizes[2]):

                    def signal(dx=dx):
                        device = (place, other, (target[2] + dx) % sizes[2])
                        pl.semaphore_signal(barrier, inc=1, device_id=device, device_id_type=MESH)

                    if dx:
                        signal()
                    else:
                        pl.when(square != 0)(signal)
                return 0

            lax.fori_loop(0, squares, greet_square, 0)

    def remote(source, target, send, recv, device):
        return pltpu.make_async_remote_copy(
            src_ref=source, dst_ref=target, send_sem=send, recv_sem=recv,
            device_id=device, device_id_type=MESH,
        )

    class Group:
        def __init__(self, source, target, send, recv, places, spared=()):
            self.spared = spared
            places = sorted(places, key=lambda place: -distance(place[0], sizes))
            self.all = [
                remote(
                    source(slot) if callable(source) else source, target.at[pl.ds(slot, 1)],
                    send, recv, against(offset),
                )
                for offset, slot in places
            ]
            self.reached = [against(offset) for offset, _ in places]
            low = min(slot for _, slot in places)
            whole = target.at[pl.ds(low, len(places))]
            self.sum = remote(whole, whole, send, recv, here)

        def start(self):
            for copy, (t, z, _) in zip(self.all, self.reached):
                if self.spared:
                    clear = [t * sizes[1] + z != square for square in self.spared]
                    pl.when(functools.reduce(jnp.logical_and, clear))(copy.start)
                else:
                    copy.start()
            return self

        def arrived(self):
            self.sum.wait_recv()

        def sent(self):
            self.sum.wait_send()

    def greet(offsets, token):
        far = [offset for offset in offsets if any(wrapped(offset))]
        for offset in far:
            pl.semaphore_signal(token, inc=1, device_id=at(offset), device_id_type=MESH)
        return len(far)

    six = [(STEPS[d], d) for d in range(6)]

    rows12 = lax.broadcasted_iota(jnp.int32, (12, 128), 0)
    chiral = jnp.where(rows12 < 6, 1.0, -1.0).astype(F32)

    def smoothed(re, im):
        return (
            PRE_SAME * re + PRE_OTHER * (chiral * im),
            PRE_SAME * im - PRE_OTHER * (chiral * re),
        )

    def send_halves(which, field):
        r0, r1, r2, r3 = (field[pl.ds(s * 3, 3), :] for s in range(4))
        i0, i1, i2, i3 = (field[pl.ds(12 + s * 3, 3), :] for s in range(4))
        for axis, lower in enumerate(
            (
                (r2, r3, i2, i3),
                (-i2, i3, r2, -r3),
                (-i3, -i2, r3, r2),
                (-r3, r2, -i3, i2),
            )
        ):
            for d in (2 * axis, 2 * axis + 1):
                for row, (up, low) in enumerate(zip((r0, r1, i0, i1), lower)):
                    value = up - low if d % 2 == 0 else up + low
                    if axis < 3:
                        half_out[which, d, pl.ds(row * 3, 3), :] = value
                    else:
                        shift = 127 if d == 6 else 1
                        halo[which, d, pl.ds(row * 3, 3), :] = pltpu.roll(value, shift, 1)

    loads[0].wait()
    first_re, first_im = smoothed(src[0:12, :], src[12:24, :])
    first[0:12, :] = first_re
    first[12:24, :] = first_im
    send_halves(0, first)
    pl.semaphore_wait(barrier, len(STEPS) + len(targets) - served.astype(jnp.int32))
    first_copies = Group(
        lambda d: half_out.at[0, pl.ds(d, 1)], halo.at[0], halo_send.at[0], halo_recv.at[0], six
    ).start()

    lanes8 = lax.broadcasted_iota(jnp.int32, (8, 128), 1)
    lane_row = lax.broadcasted_iota(jnp.int32, (1, 128), 1)
    near_blk[...] = jnp.zeros_like(near_blk)
    own_blk[...] = jnp.zeros_like(own_blk)
    around[...] = jnp.zeros_like(around)
    sum_rows[...] = jnp.zeros_like(sum_rows)
    right_rows[pl.ds(0, 1), :] = jnp.zeros((1, 128), F32)
    mv_parts[...] = jnp.zeros_like(mv_parts)
    loads[2].wait()
    per_x = bblk.shape[0] // 14

    def site_blocks(x):
        start = (x * 9) // 2
        skipped = lax.rem(x, 2) * 64
        rows = [
            [bblk[pl.ds(p * 7 * per_x + start + q, 7, stride=per_x), 0, :] for q in range(5)]
            for p in range(2)
        ]
        lane = lax.broadcasted_iota(jnp.int32, (7, 128), 1)
        for c in range(6):
            place = lax.rem(lane, 32) * 24 + 4 * c + lane // 32 + skipped
            chunk = place // 128
            within = lax.rem(place, 128)
            valid = lax.rem(lane, 32) < 24
            for p in range(2):
                value = jnp.zeros((7, 128), F32)
                for q in range(5):
                    value = jnp.where(chunk == q, lanes_from(rows[p][q], within), value)
                yield p, c, jnp.where(valid, value, 0.0)

    for p, q, value in site_blocks(here[2]):
        own_blk[0, p, q, pl.ds(0, 7), :] = value
        near_blk[p, q, pl.ds(0, 7, stride=8), :] = value
    for d in (4, 5):
        for p, q, value in site_blocks(at(STEPS[d])[2]):
            near_blk[p, q, pl.ds(1 + d, 7, stride=8), :] = value
    loads[3].wait()
    fine_f[...] = fine[...].astype(F32)
    loads[4].wait()
    for p in range(2):
        for c in range(6):
            block = mvec[pl.ds(p * 144 + c, 24, stride=6), :]
            high = block.astype(BF16)
            mv_parts[p, 0, pl.ds(0, 24), pl.ds(c * 128, 128)] = high
            mv_parts[p, 1, pl.ds(0, 24), pl.ds(c * 128, 128)] = (block - high.astype(F32)).astype(BF16)

    direction = lax.broadcasted_iota(jnp.int32, (8, 128), 0)
    is_t = direction < 2
    is_z = direction < 4
    is_x = direction < 6
    odd_one = lax.rem(direction, 2) == 1
    base = jnp.where(odd_one, 1.0, -1.0).astype(F32)
    in_z = jnp.logical_and(is_z, jnp.logical_not(is_t))
    in_x = jnp.logical_and(is_x, jnp.logical_not(is_z))
    in_y = jnp.logical_not(is_x)

    def flipped(mask):
        return jnp.where(mask, -base, base)

    sign_e = flipped(jnp.logical_or(in_z, in_x))
    sign_f = flipped(jnp.logical_or(in_z, in_y))
    sign_g = flipped(jnp.logical_or(in_x, in_y))

    def pick(a, b, c, d):
        return jnp.where(is_t, a, jnp.where(is_z, b, jnp.where(is_x, c, d)))

    loads[1].wait()

    def hopping(which):
        link = [
            [[gauge[pl.ds(p * 72 + c * 3 + e, 8, stride=9), :] for e in range(3)] for c in range(3)]
            for p in range(2)
        ]
        half = [
            [[halo[which, :, p * 6 + s * 3 + c, :] for c in range(3)] for s in range(2)]
            for p in range(2)
        ]

        def put(p, s, c, value):
            hop_rows[pl.ds(p * 12 + s * 3 + c, 1), :] = jnp.sum(value, axis=0, keepdims=True)

        for c in range(3):
            moved = [[0.0, 0.0], [0.0, 0.0]]
            for s in range(2):
                for e in range(3):
                    lr, li = link[0][c][e], link[1][c][e]
                    hr, hi = half[0][s][e], half[1][s][e]
                    moved[0][s] = moved[0][s] + (lr * hr - li * hi)
                    moved[1][s] = moved[1][s] + (lr * hi + li * hr)
            (a0, a1), (b0, b1) = moved
            put(0, 0, c, a0)
            put(0, 1, c, a1)
            put(1, 0, c, b0)
            put(1, 1, c, b1)
            put(0, 2, c, base * pick(a0, b0, b1, a1))
            put(1, 2, c, sign_e * pick(b0, a0, a1, b1))
            put(0, 3, c, sign_f * pick(a1, b1, b0, a0))
            put(1, 3, c, sign_g * pick(b1, a1, a0, b0))

    def residual(re, im):
        hop_re, hop_im = hop_rows[0:12, :], hop_rows[12:24, :]
        out_re = src[0:12, :] - (DIAGONAL * re - TWIST * (chiral * im) - 0.5 * hop_re)
        out_im = src[12:24, :] - (DIAGONAL * im + TWIST * (chiral * re) - 0.5 * hop_im)
        return out_re, out_im

    first_copies.arrived()
    near_count = greet([(2, 0, 0), (-2, 0, 0), (0, 0, 2), (0, 0, -2)], near_token)
    hopping(0)
    left_re, left_im = smoothed(*residual(first_re, first_im))
    second_re, second_im = first_re + left_re, first_im + left_im
    second[0:12, :] = second_re
    second[12:24, :] = second_im
    send_halves(1, second)
    second_copies = Group(
        lambda d: half_out.at[1, pl.ds(d, 1)], halo.at[1], halo_send.at[1], halo_recv.at[1], six
    ).start()
    blk_copies = Group(own_blk, got_blk, blk_send, blk_recv, six[:4]).start()

    second_copies.arrived()
    hopping(1)
    res_re, res_im = residual(second_re, second_im)
    res_ref[0:12, :] = res_re
    res_ref[12:24, :] = res_im
    hop_rows[0:12, :] = res_re.astype(BF16).astype(F32)
    hop_rows[12:24, :] = res_im.astype(BF16).astype(F32)

    def fine_vector(p, s, c):
        return fine_f[pl.ds(p * 288 + c * 4 + s, 24, stride=12), :]

    part_re = jnp.zeros((24, 128), F32)
    part_im = jnp.zeros((24, 128), F32)
    for s in range(4):
        for c in range(3):
            vr, vi = fine_vector(0, s, c), fine_vector(1, s, c)
            rr = hop_rows[pl.ds(s * 3 + c, 1), :]
            ri = hop_rows[pl.ds(12 + s * 3 + c, 1), :]
            part_re = part_re + (vr * rr + vi * ri)
            part_im = part_im + (vr * ri - vi * rr)
    parts = jnp.concatenate([part_re, part_im], axis=0)
    wide[0:48, :] = four_lanes(parts, 4 * lax.rem(lane_row, 32))

    def middle_row(p, c):
        rows = [wide[pl.ds(p * 24 + c * 4 + g, 1), :] for g in range(4)]
        return jnp.where(
            lane_row < 64,
            jnp.where(lane_row < 32, rows[0], rows[1]),
            jnp.where(lane_row < 96, rows[2], rows[3]),
        )

    q_re = jnp.zeros((24, 128), F32)
    q_im = jnp.zeros((24, 128), F32)
    for c in range(6):
        vr = mvec[pl.ds(c, 24, stride=6), :]
        vi = mvec[pl.ds(144 + c, 24, stride=6), :]
        mr, mi = middle_row(0, c), middle_row(1, c)
        q_re = q_re + (vr * mr + vi * mi)
        q_im = q_im + (vr * mi - vi * mr)
    sum_rows[0:24, :] = q_re
    sum_rows[32:56, :] = q_im
    right_rows[pl.ds(0, 1), pl.ds(0, 64)] = row_sums(sum_rows[...])[0:1]

    if near_count:
        pl.semaphore_wait(near_token, near_count)
    right_copies = Group(
        right_rows.at[pl.ds(0, 1)], right_rows, right_send, right_recv, [o for o in slots.items() if o[1]]
    ).start()
    final[pl.ds(96, 48), :] = 0.4 * four_lanes(parts, 4 * (lane_row // 4))
    blk_copies.arrived()
    for d in range(4):
        for p in range(2):
            for q in range(6):
                near_blk[p, q, pl.ds(1 + d, 7, stride=8), :] = got_blk[d, p, q, pl.ds(0, 7), :]
    right_copies.arrived()
    far_count = greet([(4, 0, 0), (-4, 0, 0)], far_token)

    for d in range(7):
        for i in range(7):
            slot = slots[wrapped(added(NEAR[d], NEAR[i]))]
            around[pl.ds(d * 8 + i, 1), :] = right_rows[pl.ds(slot, 1), :]
    rows_now = around[...]
    sum_re = jnp.zeros((8, 128), F32)
    sum_im = jnp.zeros((8, 128), F32)
    for c in range(6):
        xr = lanes_from(rows_now, 4 * c + lane_row // 32)
        xi = lanes_from(rows_now, 32 + 4 * c + lane_row // 32)
        br, bi = near_blk[0, c], near_blk[1, c]
        term_re = br * xr - bi * xi
        term_im = br * xi + bi * xr
        for d in range(7):
            sum_re = sum_re + term_re[d * 8:(d + 1) * 8]
            sum_im = sum_im + term_im[d * 8:(d + 1) * 8]
    right_re = lanes_from(rows_now[0:8], lax.rem(lane_row, 32))
    right_im = lanes_from(rows_now[0:8], 32 + lax.rem(lane_row, 32))
    one_re = 2.0 * right_re + four_groups(sum_re)
    one_im = 2.0 * right_im + four_groups(sum_im)

    sum_re = jnp.zeros((8, 128), F32)
    sum_im = jnp.zeros((8, 128), F32)
    for c in range(6):
        xr = lanes_from(one_re, 4 * c + lane_row // 32)
        xi = lanes_from(one_im, 4 * c + lane_row // 32)
        br, bi = own_blk[0, 0, c], own_blk[0, 1, c]
        sum_re = sum_re + (br * xr - bi * xi)
        sum_im = sum_im + (br * xi + bi * xr)
    two = four_groups(
        jnp.concatenate(
            [jnp.sum(sum_re, axis=0, keepdims=True), jnp.sum(sum_im, axis=0, keepdims=True)], axis=0
        )
    )
    fr, fi = one_re[0:1], one_im[0:1]
    sr = 2.0 * fr + two[0:1]
    si = 2.0 * fi + two[1:2]
    rr, ri = right_re[0:1], right_im[0:1]
    products = (
        fr * fr + fi * fi,
        sr * sr + si * si,
        fr * sr + fi * si,
        fr * si - fi * sr,
        fr * rr + fi * ri,
        fr * ri - fi * rr,
        sr * rr + si * ri,
        sr * ri - si * rr,
    )
    folded = jnp.concatenate(products, axis=0)
    folded = folded + pltpu.roll(folded, 16, 1)
    rows8 = lax.broadcasted_iota(jnp.int32, (8, 128), 0)
    folded = jnp.where(lanes8 // 16 == rows8, folded, 0.0)
    line_rows[pl.ds(0, 1), :] = jnp.sum(folded, axis=0, keepdims=True)
    def copy_to(target):
        t, z, x = (lax.rem(h + n - o, n) for h, o, n in zip(here, target, sizes))
        row = (t * sizes[1] + z) * sizes[2] + x
        return remote(
            line_rows.at[pl.ds(0, 1)], all_rows.at[pl.ds(row, 1), 0], all_send.at[0], all_recv.at[0], target
        )

    for target, mine in zip(targets, chosen):

        @pl.when(jnp.logical_not(mine))
        def _(target=target):
            copy_to(target).start()

    line_copies = Group(
        line_rows.at[pl.ds(0, 1)], line_rows, line_send, line_recv, [o for o in line.items() if o[1]]
    ).start()

    left = jnp.concatenate([rr, ri, fr, fi], axis=0)
    turned = jnp.concatenate([-ri, rr, -fi, fr], axis=0)
    guess = jnp.zeros((4, 768), F32)
    for p, rows in ((0, left), (1, turned)):
        high = rows.astype(BF16)
        low = (rows - high.astype(F32)).astype(BF16)
        guess = guess + jnp.dot(high[:, 0:32], mv_parts[p, 0], preferred_element_type=F32)
        guess = guess + jnp.dot(low[:, 0:32], mv_parts[p, 0], preferred_element_type=F32)
        guess = guess + jnp.dot(high[:, 0:32], mv_parts[p, 1], preferred_element_type=F32)
    mid[0] = guess
    mid_copies = Group(
        mid.at[pl.ds(0, 1)], mid, mid_send, mid_recv, [(STEPS[d], 1 + d) for d in range(4)]
    ).start()
    lanes4 = lax.broadcasted_iota(jnp.int32, (4, 128), 1)
    place4 = lax.rem(lanes4, 32)
    for c in range(6):
        now = guess[:, c * 128:(c + 1) * 128]
        mid[7, :, pl.ds(c * 128, 128)] = jnp.where(
            place4 == 31, pltpu.roll(now, 31, 1), pltpu.roll(now, 127, 1)
        )
        mid[8, :, pl.ds(c * 128, 128)] = jnp.where(
            place4 == 0, pltpu.roll(now, 97, 1), pltpu.roll(now, 1, 1)
        )
    loads[5].wait()

    def middle_step(d, sums):
        sums = list(sums)
        for c in range(6):
            br = mblk[pl.ds(d * 144 + c, 24, stride=6), :]
            bi = mblk[pl.ds((9 + d) * 144 + c, 24, stride=6), :]
            for v in range(2):
                xr = mid[d, pl.ds(2 * v, 1), pl.ds(c * 128, 128)]
                xi = mid[d, pl.ds(2 * v + 1, 1), pl.ds(c * 128, 128)]
                sums[2 * v] = sums[2 * v] + (br * xr - bi * xi)
                sums[2 * v + 1] = sums[2 * v + 1] + (br * xi + bi * xr)
        return tuple(sums)

    sums = tuple(jnp.zeros((24, 128), F32) for _ in range(4))
    sums = middle_step(0, sums)
    sums = lax.fori_loop(7, 9, middle_step, sums)

    line_copies.arrived()
    plane_rows[pl.ds(0, 1), :] = jnp.sum(line_rows[...], axis=0, keepdims=True)
    if far_count:
        pl.semaphore_wait(far_token, far_count)
    spared = [
        jnp.where(
            jnp.logical_and(here[2] == target[2], jnp.logical_not(mine)),
            target[0] * sizes[1] + target[1], -1,
        )
        for target, mine in zip(targets, chosen)
    ]
    plane_copies = Group(
        plane_rows.at[pl.ds(0, 1)], plane_rows, plane_send, plane_recv, [o for o in plane.items() if o[1]],
        spared,
    ).start()

    mid_line_copies = Group(
        mid.at[pl.ds(0, 1)], mid, mid_line_send, mid_line_recv,
        [(STEPS[d], 1 + d) for d in (4, 5)],
    ).start()
    mid_copies.arrived()
    sums = lax.fori_loop(1, 5, middle_step, sums)
    mid_line_copies.arrived()
    sums = lax.fori_loop(5, 7, middle_step, sums)
    rows24 = lax.broadcasted_iota(jnp.int32, (24, 128), 0)
    lanes24 = lax.broadcasted_iota(jnp.int32, (24, 128), 1)
    mine = lax.rem(rows24, 4) == lanes24 // 32
    for i in range(4):
        for c in range(6):
            wide[pl.ds(i * 24 + c * 4, 4), :] = jnp.broadcast_to(
                mid[0, pl.ds(i, 1), pl.ds(c * 128, 128)], (4, 128)
            )
    changes = [
        0.2 * jnp.where(mine, wide[pl.ds(i * 24, 24), :], 0.0) - 0.4 * sums[i] for i in range(4)
    ]
    final[pl.ds(0, 96), :] = lanes_from(
        four_groups(jnp.concatenate(changes, axis=0)), lane_row // 4
    )

    everyone = squares * sizes[2]

    @pl.when(served)
    def _():
        whole = all_rows.at[pl.ds(1, everyone - 1)]
        remote(whole, whole, all_send.at[0], all_recv.at[0], here).wait_recv()
        all_rows[pl.ds(0, 1)] = line_rows[pl.ds(0, 1), :].reshape(1, 1, 128)
        total_row[...] = jnp.sum(all_rows[...].reshape(everyone, 128), axis=0, keepdims=True)

    @pl.when(jnp.logical_not(served))
    def _():
        plane_copies.arrived()
        total_row[...] = jnp.sum(plane_rows[...], axis=0, keepdims=True)

    totals = jnp.broadcast_to(total_row[...], (8, 128))
    totals = jnp.sum(jnp.where(lanes8 // 16 == rows8, totals, 0.0), axis=1, keepdims=True)
    first_norm, second_norm, cross_re, cross_im, ar, ai, br, bi = (
        jnp.broadcast_to(totals[i:i + 1, :], (1, 128)) for i in range(8)
    )
    determinant = first_norm * second_norm - cross_re * cross_re - cross_im * cross_im
    one_r = (second_norm * ar - (cross_re * br - cross_im * bi)) / determinant
    one_i = (second_norm * ai - (cross_re * bi + cross_im * br)) / determinant
    two_r = (first_norm * br - (cross_re * ar + cross_im * ai)) / determinant
    two_i = (first_norm * bi - (cross_re * ai - cross_im * ar)) / determinant
    ur, ui, wr, wi = (final[pl.ds(i * 24, 24), :] for i in range(4))
    update_re = final[96:120, :] + (one_r * ur - one_i * ui) + (two_r * wr - two_i * wi)
    update_im = final[120:144, :] + (one_r * ui + one_i * ur) + (two_r * wi + two_i * wr)
    update_re = update_re.astype(BF16).astype(F32)
    update_im = update_im.astype(BF16).astype(F32)
    for s in range(4):
        for c in range(3):
            vr, vi = fine_vector(0, s, c), fine_vector(1, s, c)
            add_re = jnp.sum(vr * update_re - vi * update_im, axis=0, keepdims=True)
            add_im = jnp.sum(vr * update_im + vi * update_re, axis=0, keepdims=True)
            row = s * 3 + c
            sol_ref[pl.ds(row, 1), :] = second[pl.ds(row, 1), :] + add_re
            sol_ref[pl.ds(12 + row, 1), :] = second[pl.ds(12 + row, 1), :] + add_im

    for group in (
        first_copies, second_copies, blk_copies, right_copies, line_copies, mid_copies,
        mid_line_copies,
    ):
        group.sent()
    left_out = sum((square >= 0).astype(jnp.int32) for square in spared)
    for n in range(len(targets) + 1):

        @pl.when(left_out == n)
        def _(n=n):
            whole = plane_rows.at[pl.ds(1, squares - 1 - n)]
            remote(whole, whole, plane_send, plane_recv, here).wait_send()

    for target, mine in zip(targets, chosen):

        @pl.when(jnp.logical_not(mine))
        def _(target=target):
            copy_to(target).wait_send()


def deliver(sol_v, res_v, sol_h, res_h, sem):
    copies = (
        pltpu.make_async_copy(sol_v, sol_h, sem.at[0]),
        pltpu.make_async_copy(res_v, res_h, sem.at[1]),
    )
    for copy in copies:
        copy.start()
    for copy in copies:
        copy.wait()


def solution(mesh):
    sizes = tuple(mesh.shape[axis] for axis in ("ta", "gz", "xy"))
    slots = plan(sizes)[1]

    def shards(source_field, gauge_links, fine_vectors, middle_blocks, middle_vectors, bottom_blocks):
        fine = jnp.transpose(fine_vectors, (0, 1, 3, 4, 5, 6, 2, 7)).reshape(576, 128)
        operands = (
            source_field.reshape(24, 128),
            gauge_links.reshape(144, 128),
            fine,
            middle_blocks.reshape(2592, 128),
            middle_vectors.reshape(288, 128),
            bottom_blocks.reshape(-1, 1, 128),
        )
        vmem = [pltpu.VMEM(o.shape, o.dtype) for o in operands]
        dma = pltpu.SemaphoreType.DMA
        sol, res = pl.pallas_call(
            functools.partial(kernel, sizes),
            out_shape=(pltpu.VMEM((24, 128), F32),) * 2,
            in_specs=[pl.BlockSpec(memory_space=pltpu.HBM)] * len(operands),
            out_specs=(pl.BlockSpec(memory_space=pltpu.VMEM),) * 2,
            scratch_shapes=vmem
            + [
                pltpu.VMEM((2, 8, 12, 128), F32),
                pltpu.VMEM((2, 6, 12, 128), F32),
                pltpu.VMEM((24, 128), F32),
                pltpu.VMEM((24, 128), F32),
                pltpu.VMEM((24, 128), F32),
                pltpu.VMEM((576, 128), F32),
                pltpu.VMEM((2, 2, 32, 768), BF16),
                pltpu.VMEM((1, 2, 6, 8, 128), F32),
                pltpu.VMEM((4, 2, 6, 8, 128), F32),
                pltpu.VMEM((2, 6, 56, 128), F32),
                pltpu.VMEM((len(slots), 128), F32),
                pltpu.VMEM((64, 128), F32),
                pltpu.VMEM((56, 128), F32),
                pltpu.VMEM((sizes[0] * sizes[1], 128), F32),
                pltpu.VMEM((sizes[2], 128), F32),
                pltpu.VMEM((9, 4, 768), F32),
                pltpu.VMEM((96, 128), F32),
                pltpu.VMEM((144, 128), F32),
                dma((len(operands),)),
                dma((2,)),
                dma((2,)),
            ]
            + [dma] * 12
            + [pltpu.SemaphoreType.REGULAR] * 2
            + [
                pltpu.VMEM((sizes[0] * sizes[1] * sizes[2], 1, 128), F32),
                pltpu.VMEM((1, 128), F32),
                dma((1,)),
                dma((1,)),
            ],
            compiler_params=pltpu.CompilerParams(collective_id=0, has_side_effects=True),
        )(*operands)
        sol, res = pl.pallas_call(
            deliver,
            out_shape=(jax.ShapeDtypeStruct((24, 128), F32),) * 2,
            in_specs=[pl.BlockSpec(memory_space=pltpu.VMEM)] * 2,
            out_specs=(pl.BlockSpec(memory_space=pltpu.HBM),) * 2,
            scratch_shapes=[pltpu.SemaphoreType.DMA((2,))],
        )(*(pltpu.with_memory_space_constraint(o, pltpu.VMEM) for o in (sol, res)))
        return sol.reshape(source_field.shape), res.reshape(source_field.shape)

    return jax.shard_map(
        shards,
        mesh=mesh,
        in_specs=(
            P(None, None, None, "ta", "gz", "xy", None),
            P(None, None, None, None, "ta", "gz", "xy", None),
            P(None, None, None, None, "ta", "gz", "xy", None),
            P(None, None, None, "ta", "gz", "xy", None),
            P(None, None, "ta", "gz", "xy", None),
            P(None, None, "ta", "gz", None),
        ),
        out_specs=(
            P(None, None, None, "ta", "gz", "xy", None),
            P(None, None, None, "ta", "gz", "xy", None),
        ),
        check_vma=False,
    )
```

```python
import functools

import jax
import jax.numpy as jnp
from jax import lax
from jax.experimental import pallas as pl
from jax.experimental.pallas import tpu as pltpu
from jax.sharding import PartitionSpec as P

MESH = pl.DeviceIdType.MESH
F32 = jnp.float32
BF16 = jnp.bfloat16

DIAGONAL = 4.1
TWIST = 0.1
DENOMINATOR = DIAGONAL * DIAGONAL + TWIST * TWIST
PRE_SAME = 0.8 * DIAGONAL / DENOMINATOR
PRE_OTHER = 0.8 * TWIST / DENOMINATOR

STEPS = ((1, 0, 0), (-1, 0, 0), (0, 1, 0), (0, -1, 0), (0, 0, 1), (0, 0, -1))
NEAR = ((0, 0, 0),) + STEPS
TARGETS = ((0, 1, 0), (2, 0, 0), (2, 1, 0))


def added(one, other):
    return tuple(a + b for a, b in zip(one, other))


def plan(sizes):
    def wrapped(offset):
        return tuple(o % n for o, n in zip(offset, sizes))

    slots = {}
    for one in NEAR:
        for other in NEAR:
            slots.setdefault(wrapped(added(one, other)), len(slots))
    plane = {}
    for dt in range(sizes[0]):
        for dz in range(sizes[1]):
            plane[(dt, dz, 0)] = len(plane)
    line = {(0, 0, dx): dx for dx in range(sizes[2])}
    return wrapped, slots, plane, line


def lanes_from(value, places):
    return jnp.take_along_axis(
        value, jnp.broadcast_to(places, value.shape), axis=1, mode="promise_in_bounds"
    )


def four_groups(value):
    return (value + pltpu.roll(value, 32, 1)) + (pltpu.roll(value, 64, 1) + pltpu.roll(value, 96, 1))


def four_lanes(value, first):
    one, two, three, four = (lanes_from(value, first + b) for b in range(4))
    return (one + two) + (three + four)


def distance(offset, sizes):
    t, z, x = (min(o % n, n - o % n) for o, n in zip(offset, sizes))
    return t / 2 + (t % 2) / 2 + z + x


def kernel(
    sizes,
    src_h, gauge_h, fine_h, mblk_h, mvec_h, bblk_h,
    sol_ref, res_ref,
    src, gauge, fine, mblk, mvec, bblk,
    halo, half_out, hop_rows, first, second, fine_f, mv_parts, own_blk, got_blk, near_blk,
    right_rows, sum_rows, around, plane_rows, line_rows, mid, wide, final,
    local_sem, halo_send, halo_recv, blk_send, blk_recv, right_send, right_recv,
    plane_send, plane_recv, line_send, line_recv, mid_send, mid_recv, mid_line_send, mid_line_recv,
    near_token, far_token, all_rows, total_row, all_send, all_recv,
):
    wrapped, slots, plane, line = plan(sizes)
    here = tuple(lax.axis_index(axis) for axis in ("ta", "gz", "xy"))

    def at(offset):
        return tuple(
            h if o % n == 0 else lax.rem(h + (o % n), n) for h, o, n in zip(here, offset, sizes)
        )

    def against(offset):
        return at(tuple(-o for o in offset))

    loads = [
        pltpu.make_async_copy(a, b, local_sem.at[i])
        for i, (a, b) in enumerate(
            (
                (src_h, src), (gauge_h, gauge), (bblk_h, bblk), (fine_h, fine), (mvec_h, mvec),
                (mblk_h, mblk),
            )
        )
    ]
    barrier = pltpu.get_barrier_semaphore()
    for step in STEPS:
        pl.semaphore_signal(barrier, inc=1, device_id=at(step), device_id_type=MESH)
    for load in loads:
        load.start()

    def is_here(place):
        same = [h == o for h, o in zip(here, place)]
        return jnp.logical_and(jnp.logical_and(same[0], same[1]), same[2])

    targets = [t for t in TARGETS if all(o < n for o, n in zip(t, sizes))]
    chosen = [is_here(t) for t in targets]
    served = functools.reduce(jnp.logical_or, chosen)
    squares = sizes[0] * sizes[1]
    for target, mine in zip(targets, chosen):

        @pl.when(mine)
        def _(target=target):
            def greet_square(i, _):
                square = lax.rem(i + squares // 2, squares)
                place = lax.rem(target[0] + square // sizes[1], sizes[0])
                other = lax.rem(target[1] + lax.rem(square, sizes[1]), sizes[1])
                for dx in range(sizes[2]):

                    def signal(dx=dx):
                        device = (place, other, (target[2] + dx) % sizes[2])
                        pl.semaphore_signal(barrier, inc=1, device_id=device, device_id_type=MESH)

                    if dx:
                        signal()
                    else:
                        pl.when(square != 0)(signal)
                return 0

            lax.fori_loop(0, squares, greet_square, 0)

    def remote(source, target, send, recv, device):
        return pltpu.make_async_remote_copy(
            src_ref=source, dst_ref=target, send_sem=send, recv_sem=recv,
            device_id=device, device_id_type=MESH,
        )

    class Group:
        def __init__(self, source, target, send, recv, places, spared=()):
            self.spared = spared
            places = sorted(places, key=lambda place: -distance(place[0], sizes))
            self.all = [
                remote(
                    source(slot) if callable(source) else source, target.at[pl.ds(slot, 1)],
                    send, recv, against(offset),
                )
                for offset, slot in places
            ]
            self.reached = [against(offset) for offset, _ in places]
            low = min(slot for _, slot in places)
            whole = target.at[pl.ds(low, len(places))]
            self.sum = remote(whole, whole, send, recv, here)

        def start(self):
            for copy, (t, z, _) in zip(self.all, self.reached):
                if self.spared:
                    clear = [t * sizes[1] + z != square for square in self.spared]
                    pl.when(functools.reduce(jnp.logical_and, clear))(copy.start)
                else:
                    copy.start()
            return self

        def arrived(self):
            self.sum.wait_recv()

        def sent(self):
            self.sum.wait_send()

    def greet(offsets, token):
        far = [offset for offset in offsets if any(wrapped(offset))]
        for offset in far:
            pl.semaphore_signal(token, inc=1, device_id=at(offset), device_id_type=MESH)
        return len(far)

    six = [(STEPS[d], d) for d in range(6)]

    rows12 = lax.broadcasted_iota(jnp.int32, (12, 128), 0)
    chiral = jnp.where(rows12 < 6, 1.0, -1.0).astype(F32)

    def smoothed(re, im):
        return (
            PRE_SAME * re + PRE_OTHER * (chiral * im),
            PRE_SAME * im - PRE_OTHER * (chiral * re),
        )

    def send_halves(which, field):
        r0, r1, r2, r3 = (field[pl.ds(s * 3, 3), :] for s in range(4))
        i0, i1, i2, i3 = (field[pl.ds(12 + s * 3, 3), :] for s in range(4))
        for axis, lower in enumerate(
            (
                (r2, r3, i2, i3),
                (-i2, i3, r2, -r3),
                (-i3, -i2, r3, r2),
                (-r3, r2, -i3, i2),
            )
        ):
            for d in (2 * axis, 2 * axis + 1):
                for row, (up, low) in enumerate(zip((r0, r1, i0, i1), lower)):
                    value = up - low if d % 2 == 0 else up + low
                    if axis < 3:
                        half_out[which, d, pl.ds(row * 3, 3), :] = value
                    else:
                        shift = 127 if d == 6 else 1
                        halo[which, d, pl.ds(row * 3, 3), :] = pltpu.roll(value, shift, 1)

    loads[0].wait()
    first_re, first_im = smoothed(src[0:12, :], src[12:24, :])
    first[0:12, :] = first_re
    first[12:24, :] = first_im
    send_halves(0, first)
    pl.semaphore_wait(barrier, len(STEPS) + len(targets) - served.astype(jnp.int32))
    first_copies = Group(
        lambda d: half_out.at[0, pl.ds(d, 1)], halo.at[0], halo_send.at[0], halo_recv.at[0], six
    ).start()

    lanes8 = lax.broadcasted_iota(jnp.int32, (8, 128), 1)
    lane_row = lax.broadcasted_iota(jnp.int32, (1, 128), 1)
    near_blk[...] = jnp.zeros_like(near_blk)
    own_blk[...] = jnp.zeros_like(own_blk)
    around[...] = jnp.zeros_like(around)
    sum_rows[...] = jnp.zeros_like(sum_rows)
    right_rows[pl.ds(0, 1), :] = jnp.zeros((1, 128), F32)
    mv_parts[...] = jnp.zeros_like(mv_parts)
    loads[2].wait()
    per_x = bblk.shape[0] // 14

    def site_blocks(x):
        start = (x * 9) // 2
        skipped = lax.rem(x, 2) * 64
        rows = [
            [bblk[pl.ds(p * 7 * per_x + start + q, 7, stride=per_x), 0, :] for q in range(5)]
            for p in range(2)
        ]
        lane = lax.broadcasted_iota(jnp.int32, (7, 128), 1)
        for c in range(6):
            place = lax.rem(lane, 32) * 24 + 4 * c + lane // 32 + skipped
            chunk = place // 128
            within = lax.rem(place, 128)
            valid = lax.rem(lane, 32) < 24
            for p in range(2):
                value = jnp.zeros((7, 128), F32)
                for q in range(5):
                    value = jnp.where(chunk == q, lanes_from(rows[p][q], within), value)
                yield p, c, jnp.where(valid, value, 0.0)

    for p, q, value in site_blocks(here[2]):
        own_blk[0, p, q, pl.ds(0, 7), :] = value
        near_blk[p, q, pl.ds(0, 7, stride=8), :] = value
    for d in (4, 5):
        for p, q, value in site_blocks(at(STEPS[d])[2]):
            near_blk[p, q, pl.ds(1 + d, 7, stride=8), :] = value
    loads[3].wait()
    fine_f[...] = fine[...].astype(F32)
    loads[4].wait()
    for p in range(2):
        for c in range(6):
            block = mvec[pl.ds(p * 144 + c, 24, stride=6), :]
            high = block.astype(BF16)
            mv_parts[p, 0, pl.ds(0, 24), pl.ds(c * 128, 128)] = high
            mv_parts[p, 1, pl.ds(0, 24), pl.ds(c * 128, 128)] = (block - high.astype(F32)).astype(BF16)

    direction = lax.broadcasted_iota(jnp.int32, (8, 128), 0)
    is_t = direction < 2
    is_z = direction < 4
    is_x = direction < 6
    odd_one = lax.rem(direction, 2) == 1
    base = jnp.where(odd_one, 1.0, -1.0).astype(F32)
    in_z = jnp.logical_and(is_z, jnp.logical_not(is_t))
    in_x = jnp.logical_and(is_x, jnp.logical_not(is_z))
    in_y = jnp.logical_not(is_x)

    def flipped(mask):
        return jnp.where(mask, -base, base)

    sign_e = flipped(jnp.logical_or(in_z, in_x))
    sign_f = flipped(jnp.logical_or(in_z, in_y))
    sign_g = flipped(jnp.logical_or(in_x, in_y))

    def pick(a, b, c, d):
        return jnp.where(is_t, a, jnp.where(is_z, b, jnp.where(is_x, c, d)))

    loads[1].wait()

    def hopping(which):
        link = [
            [[gauge[pl.ds(p * 72 + c * 3 + e, 8, stride=9), :] for e in range(3)] for c in range(3)]
            for p in range(2)
        ]
        half = [
            [[halo[which, :, p * 6 + s * 3 + c, :] for c in range(3)] for s in range(2)]
            for p in range(2)
        ]

        def put(p, s, c, value):
            hop_rows[pl.ds(p * 12 + s * 3 + c, 1), :] = jnp.sum(value, axis=0, keepdims=True)

        for c in range(3):
            moved = [[0.0, 0.0], [0.0, 0.0]]
            for s in range(2):
                for e in range(3):
                    lr, li = link[0][c][e], link[1][c][e]
                    hr, hi = half[0][s][e], half[1][s][e]
                    moved[0][s] = moved[0][s] + (lr * hr - li * hi)
                    moved[1][s] = moved[1][s] + (lr * hi + li * hr)
            (a0, a1), (b0, b1) = moved
            put(0, 0, c, a0)
            put(0, 1, c, a1)
            put(1, 0, c, b0)
            put(1, 1, c, b1)
            put(0, 2, c, base * pick(a0, b0, b1, a1))
            put(1, 2, c, sign_e * pick(b0, a0, a1, b1))
            put(0, 3, c, sign_f * pick(a1, b1, b0, a0))
            put(1, 3, c, sign_g * pick(b1, a1, a0, b0))

    def residual(re, im):
        hop_re, hop_im = hop_rows[0:12, :], hop_rows[12:24, :]
        out_re = src[0:12, :] - (DIAGONAL * re - TWIST * (chiral * im) - 0.5 * hop_re)
        out_im = src[12:24, :] - (DIAGONAL * im + TWIST * (chiral * re) - 0.5 * hop_im)
        return out_re, out_im

    first_copies.arrived()
    near_count = greet([(2, 0, 0), (-2, 0, 0), (0, 0, 2), (0, 0, -2)], near_token)
    hopping(0)
    left_re, left_im = smoothed(*residual(first_re, first_im))
    second_re, second_im = first_re + left_re, first_im + left_im
    second[0:12, :] = second_re
    second[12:24, :] = second_im
    send_halves(1, second)
    second_copies = Group(
        lambda d: half_out.at[1, pl.ds(d, 1)], halo.at[1], halo_send.at[1], halo_recv.at[1], six
    ).start()
    blk_copies = Group(own_blk, got_blk, blk_send, blk_recv, six[:4]).start()

    second_copies.arrived()
    hopping(1)
    res_re, res_im = residual(second_re, second_im)
    res_ref[0:12, :] = res_re
    res_ref[12:24, :] = res_im
    hop_rows[0:12, :] = res_re.astype(BF16).astype(F32)
    hop_rows[12:24, :] = res_im.astype(BF16).astype(F32)

    def fine_vector(p, s, c):
        return fine_f[pl.ds(p * 288 + c * 4 + s, 24, stride=12), :]

    part_re = jnp.zeros((24, 128), F32)
    part_im = jnp.zeros((24, 128), F32)
    for s in range(4):
        for c in range(3):
            vr, vi = fine_vector(0, s, c), fine_vector(1, s, c)
            rr = hop_rows[pl.ds(s * 3 + c, 1), :]
            ri = hop_rows[pl.ds(12 + s * 3 + c, 1), :]
            part_re = part_re + (vr * rr + vi * ri)
            part_im = part_im + (vr * ri - vi * rr)
    parts = jnp.concatenate([part_re, part_im], axis=0)
    wide[0:48, :] = four_lanes(parts, 4 * lax.rem(lane_row, 32))

    def middle_row(p, c):
        rows = [wide[pl.ds(p * 24 + c * 4 + g, 1), :] for g in range(4)]
        return jnp.where(
            lane_row < 64,
            jnp.where(lane_row < 32, rows[0], rows[1]),
            jnp.where(lane_row < 96, rows[2], rows[3]),
        )

    q_re = jnp.zeros((24, 128), F32)
    q_im = jnp.zeros((24, 128), F32)
    for c in range(6):
        vr = mvec[pl.ds(c, 24, stride=6), :]
        vi = mvec[pl.ds(144 + c, 24, stride=6), :]
        mr, mi = middle_row(0, c), middle_row(1, c)
        q_re = q_re + (vr * mr + vi * mi)
        q_im = q_im + (vr * mi - vi * mr)
    sum_rows[0:24, :] = q_re
    sum_rows[32:56, :] = q_im
    column = jnp.sum(sum_rows[...], axis=1, keepdims=True)
    lanes64 = lax.broadcasted_iota(jnp.int32, (64, 128), 1)
    rows64 = lax.broadcasted_iota(jnp.int32, (64, 128), 0)
    right_rows[pl.ds(0, 1), :] = jnp.sum(
        jnp.where(lanes64 == rows64, column, 0.0), axis=0, keepdims=True
    )

    if near_count:
        pl.semaphore_wait(near_token, near_count)
    right_copies = Group(
        right_rows.at[pl.ds(0, 1)], right_rows, right_send, right_recv, [o for o in slots.items() if o[1]]
    ).start()
    final[pl.ds(96, 48), :] = 0.4 * four_lanes(parts, 4 * (lane_row // 4))
    blk_copies.arrived()
    for d in range(4):
        for p in range(2):
            for q in range(6):
                near_blk[p, q, pl.ds(1 + d, 7, stride=8), :] = got_blk[d, p, q, pl.ds(0, 7), :]
    right_copies.arrived()
    far_count = greet([(4, 0, 0), (-4, 0, 0)], far_token)

    for d in range(7):
        for i in range(7):
            slot = slots[wrapped(added(NEAR[d], NEAR[i]))]
            around[pl.ds(d * 8 + i, 1), :] = right_rows[pl.ds(slot, 1), :]
    rows_now = around[...]
    sum_re = jnp.zeros((8, 128), F32)
    sum_im = jnp.zeros((8, 128), F32)
    for c in range(6):
        xr = lanes_from(rows_now, 4 * c + lane_row // 32)
        xi = lanes_from(rows_now, 32 + 4 * c + lane_row // 32)
        br, bi = near_blk[0, c], near_blk[1, c]
        term_re = br * xr - bi * xi
        term_im = br * xi + bi * xr
        for d in range(7):
            sum_re = sum_re + term_re[d * 8:(d + 1) * 8]
            sum_im = sum_im + term_im[d * 8:(d + 1) * 8]
    right_re = lanes_from(rows_now[0:8], lax.rem(lane_row, 32))
    right_im = lanes_from(rows_now[0:8], 32 + lax.rem(lane_row, 32))
    one_re = 2.0 * right_re + four_groups(sum_re)
    one_im = 2.0 * right_im + four_groups(sum_im)

    sum_re = jnp.zeros((8, 128), F32)
    sum_im = jnp.zeros((8, 128), F32)
    for c in range(6):
        xr = lanes_from(one_re, 4 * c + lane_row // 32)
        xi = lanes_from(one_im, 4 * c + lane_row // 32)
        br, bi = own_blk[0, 0, c], own_blk[0, 1, c]
        sum_re = sum_re + (br * xr - bi * xi)
        sum_im = sum_im + (br * xi + bi * xr)
    two = four_groups(
        jnp.concatenate(
            [jnp.sum(sum_re, axis=0, keepdims=True), jnp.sum(sum_im, axis=0, keepdims=True)], axis=0
        )
    )
    fr, fi = one_re[0:1], one_im[0:1]
    sr = 2.0 * fr + two[0:1]
    si = 2.0 * fi + two[1:2]
    rr, ri = right_re[0:1], right_im[0:1]
    products = (
        fr * fr + fi * fi,
        sr * sr + si * si,
        fr * sr + fi * si,
        fr * si - fi * sr,
        fr * rr + fi * ri,
        fr * ri - fi * rr,
        sr * rr + si * ri,
        sr * ri - si * rr,
    )
    folded = jnp.concatenate(products, axis=0)
    folded = folded + pltpu.roll(folded, 16, 1)
    rows8 = lax.broadcasted_iota(jnp.int32, (8, 128), 0)
    folded = jnp.where(lanes8 // 16 == rows8, folded, 0.0)
    line_rows[pl.ds(0, 1), :] = jnp.sum(folded, axis=0, keepdims=True)
    def copy_to(target):
        t, z, x = (lax.rem(h + n - o, n) for h, o, n in zip(here, target, sizes))
        row = (t * sizes[1] + z) * sizes[2] + x
        return remote(
            line_rows.at[pl.ds(0, 1)], all_rows.at[pl.ds(row, 1)], all_send.at[0], all_recv.at[0], target
        )

    for target, mine in zip(targets, chosen):

        @pl.when(jnp.logical_not(mine))
        def _(target=target):
            copy_to(target).start()

    line_copies = Group(
        line_rows.at[pl.ds(0, 1)], line_rows, line_send, line_recv, [o for o in line.items() if o[1]]
    ).start()

    left = jnp.concatenate([rr, ri, fr, fi], axis=0)
    turned = jnp.concatenate([-ri, rr, -fi, fr], axis=0)
    guess = jnp.zeros((4, 768), F32)
    for p, rows in ((0, left), (1, turned)):
        high = rows.astype(BF16)
        low = (rows - high.astype(F32)).astype(BF16)
        guess = guess + jnp.dot(high[:, 0:32], mv_parts[p, 0], preferred_element_type=F32)
        guess = guess + jnp.dot(low[:, 0:32], mv_parts[p, 0], preferred_element_type=F32)
        guess = guess + jnp.dot(high[:, 0:32], mv_parts[p, 1], preferred_element_type=F32)
    mid[0] = guess
    mid_copies = Group(
        mid.at[pl.ds(0, 1)], mid, mid_send, mid_recv, [(STEPS[d], 1 + d) for d in range(4)]
    ).start()
    lanes4 = lax.broadcasted_iota(jnp.int32, (4, 128), 1)
    place4 = lax.rem(lanes4, 32)
    for c in range(6):
        now = guess[:, c * 128:(c + 1) * 128]
        mid[7, :, pl.ds(c * 128, 128)] = jnp.where(
            place4 == 31, pltpu.roll(now, 31, 1), pltpu.roll(now, 127, 1)
        )
        mid[8, :, pl.ds(c * 128, 128)] = jnp.where(
            place4 == 0, pltpu.roll(now, 97, 1), pltpu.roll(now, 1, 1)
        )
    loads[5].wait()

    def middle_step(d, sums):
        sums = list(sums)
        for c in range(6):
            br = mblk[pl.ds(d * 144 + c, 24, stride=6), :]
            bi = mblk[pl.ds((9 + d) * 144 + c, 24, stride=6), :]
            for v in range(2):
                xr = mid[d, pl.ds(2 * v, 1), pl.ds(c * 128, 128)]
                xi = mid[d, pl.ds(2 * v + 1, 1), pl.ds(c * 128, 128)]
                sums[2 * v] = sums[2 * v] + (br * xr - bi * xi)
                sums[2 * v + 1] = sums[2 * v + 1] + (br * xi + bi * xr)
        return tuple(sums)

    sums = tuple(jnp.zeros((24, 128), F32) for _ in range(4))
    sums = middle_step(0, sums)
    sums = lax.fori_loop(7, 9, middle_step, sums)

    line_copies.arrived()
    plane_rows[pl.ds(0, 1), :] = jnp.sum(line_rows[...], axis=0, keepdims=True)
    if far_count:
        pl.semaphore_wait(far_token, far_count)
    spared = [
        jnp.where(
            jnp.logical_and(here[2] == target[2], jnp.logical_not(mine)),
            target[0] * sizes[1] + target[1], -1,
        )
        for target, mine in zip(targets, chosen)
    ]
    plane_copies = Group(
        plane_rows.at[pl.ds(0, 1)], plane_rows, plane_send, plane_recv, [o for o in plane.items() if o[1]],
        spared,
    ).start()

    mid_line_copies = Group(
        mid.at[pl.ds(0, 1)], mid, mid_line_send, mid_line_recv,
        [(STEPS[d], 1 + d) for d in (4, 5)],
    ).start()
    mid_copies.arrived()
    sums = lax.fori_loop(1, 5, middle_step, sums)
    mid_line_copies.arrived()
    sums = lax.fori_loop(5, 7, middle_step, sums)
    rows24 = lax.broadcasted_iota(jnp.int32, (24, 128), 0)
    lanes24 = lax.broadcasted_iota(jnp.int32, (24, 128), 1)
    mine = lax.rem(rows24, 4) == lanes24 // 32
    for i in range(4):
        for c in range(6):
            wide[pl.ds(i * 24 + c * 4, 4), :] = jnp.broadcast_to(
                mid[0, pl.ds(i, 1), pl.ds(c * 128, 128)], (4, 128)
            )
    changes = [
        0.2 * jnp.where(mine, wide[pl.ds(i * 24, 24), :], 0.0) - 0.4 * sums[i] for i in range(4)
    ]
    final[pl.ds(0, 96), :] = lanes_from(
        four_groups(jnp.concatenate(changes, axis=0)), lane_row // 4
    )

    everyone = squares * sizes[2]

    @pl.when(served)
    def _():
        whole = all_rows.at[pl.ds(1, everyone - 1)]
        remote(whole, whole, all_send.at[0], all_recv.at[0], here).wait_recv()
        all_rows[pl.ds(0, 1), :] = line_rows[pl.ds(0, 1), :]
        total_row[...] = jnp.sum(all_rows[...], axis=0, keepdims=True)

    @pl.when(jnp.logical_not(served))
    def _():
        plane_copies.arrived()
        total_row[...] = jnp.sum(plane_rows[...], axis=0, keepdims=True)

    totals = jnp.broadcast_to(total_row[...], (8, 128))
    totals = jnp.sum(jnp.where(lanes8 // 16 == rows8, totals, 0.0), axis=1, keepdims=True)
    first_norm, second_norm, cross_re, cross_im, ar, ai, br, bi = (
        jnp.broadcast_to(totals[i:i + 1, :], (1, 128)) for i in range(8)
    )
    determinant = first_norm * second_norm - cross_re * cross_re - cross_im * cross_im
    one_r = (second_norm * ar - (cross_re * br - cross_im * bi)) / determinant
    one_i = (second_norm * ai - (cross_re * bi + cross_im * br)) / determinant
    two_r = (first_norm * br - (cross_re * ar + cross_im * ai)) / determinant
    two_i = (first_norm * bi - (cross_re * ai - cross_im * ar)) / determinant
    ur, ui, wr, wi = (final[pl.ds(i * 24, 24), :] for i in range(4))
    update_re = final[96:120, :] + (one_r * ur - one_i * ui) + (two_r * wr - two_i * wi)
    update_im = final[120:144, :] + (one_r * ui + one_i * ur) + (two_r * wi + two_i * wr)
    update_re = update_re.astype(BF16).astype(F32)
    update_im = update_im.astype(BF16).astype(F32)
    for s in range(4):
        for c in range(3):
            vr, vi = fine_vector(0, s, c), fine_vector(1, s, c)
            add_re = jnp.sum(vr * update_re - vi * update_im, axis=0, keepdims=True)
            add_im = jnp.sum(vr * update_im + vi * update_re, axis=0, keepdims=True)
            row = s * 3 + c
            sol_ref[pl.ds(row, 1), :] = second[pl.ds(row, 1), :] + add_re
            sol_ref[pl.ds(12 + row, 1), :] = second[pl.ds(12 + row, 1), :] + add_im

    for group in (
        first_copies, second_copies, blk_copies, right_copies, line_copies, mid_copies,
        mid_line_copies,
    ):
        group.sent()
    left_out = sum((square >= 0).astype(jnp.int32) for square in spared)
    for n in range(len(targets) + 1):

        @pl.when(left_out == n)
        def _(n=n):
            whole = plane_rows.at[pl.ds(1, squares - 1 - n)]
            remote(whole, whole, plane_send, plane_recv, here).wait_send()

    for target, mine in zip(targets, chosen):

        @pl.when(jnp.logical_not(mine))
        def _(target=target):
            copy_to(target).wait_send()


def deliver(sol_v, res_v, sol_h, res_h, sem):
    copies = (
        pltpu.make_async_copy(sol_v, sol_h, sem.at[0]),
        pltpu.make_async_copy(res_v, res_h, sem.at[1]),
    )
    for copy in copies:
        copy.start()
    for copy in copies:
        copy.wait()


def solution(mesh):
    sizes = tuple(mesh.shape[axis] for axis in ("ta", "gz", "xy"))
    slots = plan(sizes)[1]

    def shards(source_field, gauge_links, fine_vectors, middle_blocks, middle_vectors, bottom_blocks):
        fine = jnp.transpose(fine_vectors, (0, 1, 3, 4, 5, 6, 2, 7)).reshape(576, 128)
        operands = (
            source_field.reshape(24, 128),
            gauge_links.reshape(144, 128),
            fine,
            middle_blocks.reshape(2592, 128),
            middle_vectors.reshape(288, 128),
            bottom_blocks.reshape(-1, 1, 128),
        )
        vmem = [pltpu.VMEM(o.shape, o.dtype) for o in operands]
        dma = pltpu.SemaphoreType.DMA
        sol, res = pl.pallas_call(
            functools.partial(kernel, sizes),
            out_shape=(pltpu.VMEM((24, 128), F32),) * 2,
            in_specs=[pl.BlockSpec(memory_space=pltpu.HBM)] * len(operands),
            out_specs=(pl.BlockSpec(memory_space=pltpu.VMEM),) * 2,
            scratch_shapes=vmem
            + [
                pltpu.VMEM((2, 8, 12, 128), F32),
                pltpu.VMEM((2, 6, 12, 128), F32),
                pltpu.VMEM((24, 128), F32),
                pltpu.VMEM((24, 128), F32),
                pltpu.VMEM((24, 128), F32),
                pltpu.VMEM((576, 128), F32),
                pltpu.VMEM((2, 2, 32, 768), BF16),
                pltpu.VMEM((1, 2, 6, 8, 128), F32),
                pltpu.VMEM((4, 2, 6, 8, 128), F32),
                pltpu.VMEM((2, 6, 56, 128), F32),
                pltpu.VMEM((len(slots), 128), F32),
                pltpu.VMEM((64, 128), F32),
                pltpu.VMEM((56, 128), F32),
                pltpu.VMEM((sizes[0] * sizes[1], 128), F32),
                pltpu.VMEM((sizes[2], 128), F32),
                pltpu.VMEM((9, 4, 768), F32),
                pltpu.VMEM((96, 128), F32),
                pltpu.VMEM((144, 128), F32),
                dma((len(operands),)),
                dma((2,)),
                dma((2,)),
            ]
            + [dma] * 12
            + [pltpu.SemaphoreType.REGULAR] * 2
            + [
                pltpu.VMEM((sizes[0] * sizes[1] * sizes[2], 128), F32),
                pltpu.VMEM((1, 128), F32),
                dma((1,)),
                dma((1,)),
            ],
            compiler_params=pltpu.CompilerParams(collective_id=0, has_side_effects=True),
        )(*operands)
        sol, res = pl.pallas_call(
            deliver,
            out_shape=(jax.ShapeDtypeStruct((24, 128), F32),) * 2,
            in_specs=[pl.BlockSpec(memory_space=pltpu.VMEM)] * 2,
            out_specs=(pl.BlockSpec(memory_space=pltpu.HBM),) * 2,
            scratch_shapes=[pltpu.SemaphoreType.DMA((2,))],
        )(*(pltpu.with_memory_space_constraint(o, pltpu.VMEM) for o in (sol, res)))
        return sol.reshape(source_field.shape), res.reshape(source_field.shape)

    return jax.shard_map(
        shards,
        mesh=mesh,
        in_specs=(
            P(None, None, None, "ta", "gz", "xy", None),
            P(None, None, None, None, "ta", "gz", "xy", None),
            P(None, None, None, None, "ta", "gz", "xy", None),
            P(None, None, None, "ta", "gz", "xy", None),
            P(None, None, "ta", "gz", "xy", None),
            P(None, None, "ta", "gz", None),
        ),
        out_specs=(
            P(None, None, None, "ta", "gz", "xy", None),
            P(None, None, None, "ta", "gz", "xy", None),
        ),
        check_vma=False,
    )
```

```python
import functools

import jax
import jax.numpy as jnp
from jax import lax
from jax.experimental import pallas as pl
from jax.experimental.pallas import tpu as pltpu
from jax.sharding import PartitionSpec as P

MESH = pl.DeviceIdType.MESH
F32 = jnp.float32
BF16 = jnp.bfloat16

DIAGONAL = 4.1
TWIST = 0.1
DENOMINATOR = DIAGONAL * DIAGONAL + TWIST * TWIST
PRE_SAME = 0.8 * DIAGONAL / DENOMINATOR
PRE_OTHER = 0.8 * TWIST / DENOMINATOR

STEPS = ((1, 0, 0), (-1, 0, 0), (0, 1, 0), (0, -1, 0), (0, 0, 1), (0, 0, -1))
NEAR = ((0, 0, 0),) + STEPS
TARGETS = ((0, 1, 0), (2, 0, 0), (2, 1, 0))


def added(one, other):
    return tuple(a + b for a, b in zip(one, other))


def plan(sizes):
    def wrapped(offset):
        return tuple(o % n for o, n in zip(offset, sizes))

    slots = {}
    for one in NEAR:
        for other in NEAR:
            slots.setdefault(wrapped(added(one, other)), len(slots))
    plane = {}
    for dt in range(sizes[0]):
        for dz in range(sizes[1]):
            plane[(dt, dz, 0)] = len(plane)
    line = {(0, 0, dx): dx for dx in range(sizes[2])}
    return wrapped, slots, plane, line


def lanes_from(value, places):
    return jnp.take_along_axis(
        value, jnp.broadcast_to(places, value.shape), axis=1, mode="promise_in_bounds"
    )


def four_groups(value):
    return (value + pltpu.roll(value, 32, 1)) + (pltpu.roll(value, 64, 1) + pltpu.roll(value, 96, 1))


def four_lanes(value, first):
    one, two, three, four = (lanes_from(value, first + b) for b in range(4))
    return (one + two) + (three + four)


def distance(offset, sizes):
    t, z, x = (min(o % n, n - o % n) for o, n in zip(offset, sizes))
    return t / 2 + (t % 2) / 2 + z + x


def kernel(
    sizes,
    src_h, gauge_h, fine_h, mblk_h, mvec_h, bblk_h,
    sol_ref, res_ref,
    src, gauge, fine, mblk, mvec, bblk,
    halo, half_out, hop_rows, first, second, fine_f, mv_parts, own_blk, got_blk, near_blk,
    right_rows, sum_rows, around, plane_rows, line_rows, mid, wide, final,
    local_sem, halo_send, halo_recv, blk_send, blk_recv, right_send, right_recv,
    plane_send, plane_recv, line_send, line_recv, mid_send, mid_recv, mid_line_send, mid_line_recv,
    near_token, far_token, all_rows, total_row, all_send, all_recv,
):
    wrapped, slots, plane, line = plan(sizes)
    here = tuple(lax.axis_index(axis) for axis in ("ta", "gz", "xy"))

    def at(offset):
        return tuple(
            h if o % n == 0 else lax.rem(h + (o % n), n) for h, o, n in zip(here, offset, sizes)
        )

    def against(offset):
        return at(tuple(-o for o in offset))

    loads = [
        pltpu.make_async_copy(a, b, local_sem.at[i])
        for i, (a, b) in enumerate(
            (
                (src_h, src), (gauge_h, gauge), (bblk_h, bblk), (fine_h, fine), (mvec_h, mvec),
                (mblk_h, mblk),
            )
        )
    ]
    barrier = pltpu.get_barrier_semaphore()
    for step in STEPS:
        pl.semaphore_signal(barrier, inc=1, device_id=at(step), device_id_type=MESH)
    for load in loads:
        load.start()

    def is_here(place):
        same = [h == o for h, o in zip(here, place)]
        return jnp.logical_and(jnp.logical_and(same[0], same[1]), same[2])

    targets = [t for t in TARGETS if all(o < n for o, n in zip(t, sizes))]
    chosen = [is_here(t) for t in targets]
    served = functools.reduce(jnp.logical_or, chosen)
    squares = sizes[0] * sizes[1]
    for target, mine in zip(targets, chosen):

        @pl.when(mine)
        def _(target=target):
            def greet_square(i, _):
                square = lax.rem(i + squares // 2, squares)
                place = lax.rem(target[0] + square // sizes[1], sizes[0])
                other = lax.rem(target[1] + lax.rem(square, sizes[1]), sizes[1])
                for dx in range(sizes[2]):

                    def signal(dx=dx):
                        device = (place, other, (target[2] + dx) % sizes[2])
                        pl.semaphore_signal(barrier, inc=1, device_id=device, device_id_type=MESH)

                    if dx:
                        signal()
                    else:
                        pl.when(square != 0)(signal)
                return 0

            lax.fori_loop(0, squares, greet_square, 0)

    def remote(source, target, send, recv, device):
        return pltpu.make_async_remote_copy(
            src_ref=source, dst_ref=target, send_sem=send, recv_sem=recv,
            device_id=device, device_id_type=MESH,
        )

    class Group:
        def __init__(self, source, target, send, recv, places, spared=()):
            self.spared = spared
            places = sorted(places, key=lambda place: -distance(place[0], sizes))
            self.all = [
                remote(
                    source(slot) if callable(source) else source, target.at[pl.ds(slot, 1)],
                    send, recv, against(offset),
                )
                for offset, slot in places
            ]
            self.reached = [against(offset) for offset, _ in places]
            low = min(slot for _, slot in places)
            whole = target.at[pl.ds(low, len(places))]
            self.sum = remote(whole, whole, send, recv, here)

        def start(self):
            for copy, (t, z, _) in zip(self.all, self.reached):
                if self.spared:
                    clear = [t * sizes[1] + z != square for square in self.spared]
                    pl.when(functools.reduce(jnp.logical_and, clear))(copy.start)
                else:
                    copy.start()
            return self

        def arrived(self):
            self.sum.wait_recv()

        def sent(self):
            self.sum.wait_send()

    def greet(offsets, token):
        far = [offset for offset in offsets if any(wrapped(offset))]
        for offset in far:
            pl.semaphore_signal(token, inc=1, device_id=at(offset), device_id_type=MESH)
        return len(far)

    six = [(STEPS[d], d) for d in range(6)]

    rows12 = lax.broadcasted_iota(jnp.int32, (12, 128), 0)
    chiral = jnp.where(rows12 < 6, 1.0, -1.0).astype(F32)

    def smoothed(re, im):
        return (
            PRE_SAME * re + PRE_OTHER * (chiral * im),
            PRE_SAME * im - PRE_OTHER * (chiral * re),
        )

    def send_halves(which, field):
        r0, r1, r2, r3 = (field[pl.ds(s * 3, 3), :] for s in range(4))
        i0, i1, i2, i3 = (field[pl.ds(12 + s * 3, 3), :] for s in range(4))
        for axis, lower in enumerate(
            (
                (r2, r3, i2, i3),
                (-i2, i3, r2, -r3),
                (-i3, -i2, r3, r2),
                (-r3, r2, -i3, i2),
            )
        ):
            for d in (2 * axis, 2 * axis + 1):
                for row, (up, low) in enumerate(zip((r0, r1, i0, i1), lower)):
                    value = up - low if d % 2 == 0 else up + low
                    if axis < 3:
                        half_out[which, d, pl.ds(row * 3, 3), :] = value
                    else:
                        shift = 127 if d == 6 else 1
                        halo[which, d, pl.ds(row * 3, 3), :] = pltpu.roll(value, shift, 1)

    loads[0].wait()
    first_re, first_im = smoothed(src[0:12, :], src[12:24, :])
    first[0:12, :] = first_re
    first[12:24, :] = first_im
    send_halves(0, first)
    pl.semaphore_wait(barrier, len(STEPS) + len(targets) - served.astype(jnp.int32))
    first_copies = Group(
        lambda d: half_out.at[0, pl.ds(d, 1)], halo.at[0], halo_send.at[0], halo_recv.at[0], six
    ).start()

    lanes8 = lax.broadcasted_iota(jnp.int32, (8, 128), 1)
    lane_row = lax.broadcasted_iota(jnp.int32, (1, 128), 1)
    near_blk[...] = jnp.zeros_like(near_blk)
    own_blk[...] = jnp.zeros_like(own_blk)
    around[...] = jnp.zeros_like(around)
    sum_rows[...] = jnp.zeros_like(sum_rows)
    right_rows[pl.ds(0, 1), :] = jnp.zeros((1, 128), F32)
    mv_parts[...] = jnp.zeros_like(mv_parts)
    loads[2].wait()
    per_x = bblk.shape[0] // 14

    def site_blocks(x):
        start = (x * 9) // 2
        skipped = lax.rem(x, 2) * 64
        rows = [
            [bblk[pl.ds(p * 7 * per_x + start + q, 7, stride=per_x), 0, :] for q in range(5)]
            for p in range(2)
        ]
        lane = lax.broadcasted_iota(jnp.int32, (7, 128), 1)
        for c in range(6):
            place = lax.rem(lane, 32) * 24 + 4 * c + lane // 32 + skipped
            chunk = place // 128
            within = lax.rem(place, 128)
            valid = lax.rem(lane, 32) < 24
            for p in range(2):
                value = jnp.zeros((7, 128), F32)
                for q in range(5):
                    value = jnp.where(chunk == q, lanes_from(rows[p][q], within), value)
                yield p, c, jnp.where(valid, value, 0.0)

    for p, q, value in site_blocks(here[2]):
        own_blk[0, p, q, pl.ds(0, 7), :] = value
        near_blk[p, q, pl.ds(0, 7, stride=8), :] = value
    for d in (4, 5):
        for p, q, value in site_blocks(at(STEPS[d])[2]):
            near_blk[p, q, pl.ds(1 + d, 7, stride=8), :] = value
    loads[3].wait()
    fine_f[...] = fine[...].astype(F32)
    loads[4].wait()
    for p in range(2):
        for c in range(6):
            block = mvec[pl.ds(p * 144 + c, 24, stride=6), :]
            high = block.astype(BF16)
            mv_parts[p, 0, pl.ds(0, 24), pl.ds(c * 128, 128)] = high
            mv_parts[p, 1, pl.ds(0, 24), pl.ds(c * 128, 128)] = (block - high.astype(F32)).astype(BF16)

    direction = lax.broadcasted_iota(jnp.int32, (8, 128), 0)
    is_t = direction < 2
    is_z = direction < 4
    is_x = direction < 6
    odd_one = lax.rem(direction, 2) == 1
    base = jnp.where(odd_one, 1.0, -1.0).astype(F32)
    in_z = jnp.logical_and(is_z, jnp.logical_not(is_t))
    in_x = jnp.logical_and(is_x, jnp.logical_not(is_z))
    in_y = jnp.logical_not(is_x)

    def flipped(mask):
        return jnp.where(mask, -base, base)

    sign_e = flipped(jnp.logical_or(in_z, in_x))
    sign_f = flipped(jnp.logical_or(in_z, in_y))
    sign_g = flipped(jnp.logical_or(in_x, in_y))

    def pick(a, b, c, d):
        return jnp.where(is_t, a, jnp.where(is_z, b, jnp.where(is_x, c, d)))

    loads[1].wait()

    link = [
        [[gauge[pl.ds(p * 72 + c * 3 + e, 8, stride=9), :] for e in range(3)] for c in range(3)]
        for p in range(2)
    ]

    def hopping(which):
        half = [
            [[halo[which, :, p * 6 + s * 3 + c, :] for c in range(3)] for s in range(2)]
            for p in range(2)
        ]

        def put(p, s, c, value):
            hop_rows[pl.ds(p * 12 + s * 3 + c, 1), :] = jnp.sum(value, axis=0, keepdims=True)

        for c in range(3):
            moved = [[0.0, 0.0], [0.0, 0.0]]
            for s in range(2):
                for e in range(3):
                    lr, li = link[0][c][e], link[1][c][e]
                    hr, hi = half[0][s][e], half[1][s][e]
                    moved[0][s] = moved[0][s] + (lr * hr - li * hi)
                    moved[1][s] = moved[1][s] + (lr * hi + li * hr)
            (a0, a1), (b0, b1) = moved
            put(0, 0, c, a0)
            put(0, 1, c, a1)
            put(1, 0, c, b0)
            put(1, 1, c, b1)
            put(0, 2, c, base * pick(a0, b0, b1, a1))
            put(1, 2, c, sign_e * pick(b0, a0, a1, b1))
            put(0, 3, c, sign_f * pick(a1, b1, b0, a0))
            put(1, 3, c, sign_g * pick(b1, a1, a0, b0))

    def residual(re, im):
        hop_re, hop_im = hop_rows[0:12, :], hop_rows[12:24, :]
        out_re = src[0:12, :] - (DIAGONAL * re - TWIST * (chiral * im) - 0.5 * hop_re)
        out_im = src[12:24, :] - (DIAGONAL * im + TWIST * (chiral * re) - 0.5 * hop_im)
        return out_re, out_im

    first_copies.arrived()
    near_count = greet([(2, 0, 0), (-2, 0, 0), (0, 0, 2), (0, 0, -2)], near_token)
    hopping(0)
    left_re, left_im = smoothed(*residual(first_re, first_im))
    second_re, second_im = first_re + left_re, first_im + left_im
    second[0:12, :] = second_re
    second[12:24, :] = second_im
    send_halves(1, second)
    second_copies = Group(
        lambda d: half_out.at[1, pl.ds(d, 1)], halo.at[1], halo_send.at[1], halo_recv.at[1], six
    ).start()
    blk_copies = Group(own_blk, got_blk, blk_send, blk_recv, six[:4]).start()

    second_copies.arrived()
    hopping(1)
    res_re, res_im = residual(second_re, second_im)
    hop_rows[0:12, :] = res_re.astype(BF16).astype(F32)
    hop_rows[12:24, :] = res_im.astype(BF16).astype(F32)

    def fine_vector(p, s, c):
        return fine_f[pl.ds(p * 288 + c * 4 + s, 24, stride=12), :]

    part_re = jnp.zeros((24, 128), F32)
    part_im = jnp.zeros((24, 128), F32)
    for s in range(4):
        for c in range(3):
            vr, vi = fine_vector(0, s, c), fine_vector(1, s, c)
            rr = hop_rows[pl.ds(s * 3 + c, 1), :]
            ri = hop_rows[pl.ds(12 + s * 3 + c, 1), :]
            part_re = part_re + (vr * rr + vi * ri)
            part_im = part_im + (vr * ri - vi * rr)
    parts = jnp.concatenate([part_re, part_im], axis=0)
    wide[0:48, :] = four_lanes(parts, 4 * lax.rem(lane_row, 32))

    def middle_row(p, c):
        rows = [wide[pl.ds(p * 24 + c * 4 + g, 1), :] for g in range(4)]
        return jnp.where(
            lane_row < 64,
            jnp.where(lane_row < 32, rows[0], rows[1]),
            jnp.where(lane_row < 96, rows[2], rows[3]),
        )

    q_re = jnp.zeros((24, 128), F32)
    q_im = jnp.zeros((24, 128), F32)
    for c in range(6):
        vr = mvec[pl.ds(c, 24, stride=6), :]
        vi = mvec[pl.ds(144 + c, 24, stride=6), :]
        mr, mi = middle_row(0, c), middle_row(1, c)
        q_re = q_re + (vr * mr + vi * mi)
        q_im = q_im + (vr * mi - vi * mr)
    sum_rows[0:24, :] = q_re
    sum_rows[32:56, :] = q_im
    column = jnp.sum(sum_rows[...], axis=1, keepdims=True)
    lanes64 = lax.broadcasted_iota(jnp.int32, (64, 128), 1)
    rows64 = lax.broadcasted_iota(jnp.int32, (64, 128), 0)
    right_rows[pl.ds(0, 1), :] = jnp.sum(
        jnp.where(lanes64 == rows64, column, 0.0), axis=0, keepdims=True
    )

    if near_count:
        pl.semaphore_wait(near_token, near_count)
    right_copies = Group(
        right_rows.at[pl.ds(0, 1)], right_rows, right_send, right_recv, [o for o in slots.items() if o[1]]
    ).start()
    res_ref[0:12, :] = res_re
    res_ref[12:24, :] = res_im
    final[pl.ds(96, 48), :] = 0.4 * four_lanes(parts, 4 * (lane_row // 4))
    blk_copies.arrived()
    for d in range(4):
        for p in range(2):
            for q in range(6):
                near_blk[p, q, pl.ds(1 + d, 7, stride=8), :] = got_blk[d, p, q, pl.ds(0, 7), :]
    right_copies.arrived()
    far_count = greet([(4, 0, 0), (-4, 0, 0)], far_token)

    for d in range(7):
        for i in range(7):
            slot = slots[wrapped(added(NEAR[d], NEAR[i]))]
            around[pl.ds(d * 8 + i, 1), :] = right_rows[pl.ds(slot, 1), :]
    rows_now = around[...]
    sum_re = jnp.zeros((8, 128), F32)
    sum_im = jnp.zeros((8, 128), F32)
    for c in range(6):
        xr = lanes_from(rows_now, 4 * c + lane_row // 32)
        xi = lanes_from(rows_now, 32 + 4 * c + lane_row // 32)
        br, bi = near_blk[0, c], near_blk[1, c]
        term_re = br * xr - bi * xi
        term_im = br * xi + bi * xr
        for d in range(7):
            sum_re = sum_re + term_re[d * 8:(d + 1) * 8]
            sum_im = sum_im + term_im[d * 8:(d + 1) * 8]
    right_re = lanes_from(rows_now[0:8], lax.rem(lane_row, 32))
    right_im = lanes_from(rows_now[0:8], 32 + lax.rem(lane_row, 32))
    one_re = 2.0 * right_re + four_groups(sum_re)
    one_im = 2.0 * right_im + four_groups(sum_im)

    sum_re = jnp.zeros((8, 128), F32)
    sum_im = jnp.zeros((8, 128), F32)
    for c in range(6):
        xr = lanes_from(one_re, 4 * c + lane_row // 32)
        xi = lanes_from(one_im, 4 * c + lane_row // 32)
        br, bi = own_blk[0, 0, c], own_blk[0, 1, c]
        sum_re = sum_re + (br * xr - bi * xi)
        sum_im = sum_im + (br * xi + bi * xr)
    two = four_groups(
        jnp.concatenate(
            [jnp.sum(sum_re, axis=0, keepdims=True), jnp.sum(sum_im, axis=0, keepdims=True)], axis=0
        )
    )
    fr, fi = one_re[0:1], one_im[0:1]
    sr = 2.0 * fr + two[0:1]
    si = 2.0 * fi + two[1:2]
    rr, ri = right_re[0:1], right_im[0:1]
    products = (
        fr * fr + fi * fi,
        sr * sr + si * si,
        fr * sr + fi * si,
        fr * si - fi * sr,
        fr * rr + fi * ri,
        fr * ri - fi * rr,
        sr * rr + si * ri,
        sr * ri - si * rr,
    )
    folded = jnp.concatenate(products, axis=0)
    folded = folded + pltpu.roll(folded, 16, 1)
    rows8 = lax.broadcasted_iota(jnp.int32, (8, 128), 0)
    folded = jnp.where(lanes8 // 16 == rows8, folded, 0.0)
    line_rows[pl.ds(0, 1), :] = jnp.sum(folded, axis=0, keepdims=True)
    def copy_to(target):
        t, z, x = (lax.rem(h + n - o, n) for h, o, n in zip(here, target, sizes))
        row = (t * sizes[1] + z) * sizes[2] + x
        return remote(
            line_rows.at[pl.ds(0, 1)], all_rows.at[pl.ds(row, 1)], all_send.at[0], all_recv.at[0], target
        )

    for target, mine in zip(targets, chosen):

        @pl.when(jnp.logical_not(mine))
        def _(target=target):
            copy_to(target).start()

    line_copies = Group(
        line_rows.at[pl.ds(0, 1)], line_rows, line_send, line_recv, [o for o in line.items() if o[1]]
    ).start()

    left = jnp.concatenate([rr, ri, fr, fi], axis=0)
    turned = jnp.concatenate([-ri, rr, -fi, fr], axis=0)
    guess = jnp.zeros((4, 768), F32)
    for p, rows in ((0, left), (1, turned)):
        high = rows.astype(BF16)
        low = (rows - high.astype(F32)).astype(BF16)
        guess = guess + jnp.dot(high[:, 0:32], mv_parts[p, 0], preferred_element_type=F32)
        guess = guess + jnp.dot(low[:, 0:32], mv_parts[p, 0], preferred_element_type=F32)
        guess = guess + jnp.dot(high[:, 0:32], mv_parts[p, 1], preferred_element_type=F32)
    mid[0] = guess
    mid_copies = Group(
        mid.at[pl.ds(0, 1)], mid, mid_send, mid_recv, [(STEPS[d], 1 + d) for d in range(4)]
    ).start()
    lanes4 = lax.broadcasted_iota(jnp.int32, (4, 128), 1)
    place4 = lax.rem(lanes4, 32)
    for c in range(6):
        now = guess[:, c * 128:(c + 1) * 128]
        mid[7, :, pl.ds(c * 128, 128)] = jnp.where(
            place4 == 31, pltpu.roll(now, 31, 1), pltpu.roll(now, 127, 1)
        )
        mid[8, :, pl.ds(c * 128, 128)] = jnp.where(
            place4 == 0, pltpu.roll(now, 97, 1), pltpu.roll(now, 1, 1)
        )
    loads[5].wait()

    def middle_step(d, sums):
        sums = list(sums)
        for c in range(6):
            br = mblk[pl.ds(d * 144 + c, 24, stride=6), :]
            bi = mblk[pl.ds((9 + d) * 144 + c, 24, stride=6), :]
            for v in range(2):
                xr = mid[d, pl.ds(2 * v, 1), pl.ds(c * 128, 128)]
                xi = mid[d, pl.ds(2 * v + 1, 1), pl.ds(c * 128, 128)]
                sums[2 * v] = sums[2 * v] + (br * xr - bi * xi)
                sums[2 * v + 1] = sums[2 * v + 1] + (br * xi + bi * xr)
        return tuple(sums)

    sums = tuple(jnp.zeros((24, 128), F32) for _ in range(4))
    sums = middle_step(0, sums)
    sums = lax.fori_loop(7, 9, middle_step, sums)

    line_copies.arrived()
    plane_rows[pl.ds(0, 1), :] = jnp.sum(line_rows[...], axis=0, keepdims=True)
    if far_count:
        pl.semaphore_wait(far_token, far_count)
    spared = [
        jnp.where(
            jnp.logical_and(here[2] == target[2], jnp.logical_not(mine)),
            target[0] * sizes[1] + target[1], -1,
        )
        for target, mine in zip(targets, chosen)
    ]
    plane_copies = Group(
        plane_rows.at[pl.ds(0, 1)], plane_rows, plane_send, plane_recv, [o for o in plane.items() if o[1]],
        spared,
    ).start()

    mid_line_copies = Group(
        mid.at[pl.ds(0, 1)], mid, mid_line_send, mid_line_recv,
        [(STEPS[d], 1 + d) for d in (4, 5)],
    ).start()
    mid_copies.arrived()
    sums = lax.fori_loop(1, 5, middle_step, sums)
    mid_line_copies.arrived()
    sums = lax.fori_loop(5, 7, middle_step, sums)
    rows24 = lax.broadcasted_iota(jnp.int32, (24, 128), 0)
    lanes24 = lax.broadcasted_iota(jnp.int32, (24, 128), 1)
    mine = lax.rem(rows24, 4) == lanes24 // 32
    for i in range(4):
        for c in range(6):
            wide[pl.ds(i * 24 + c * 4, 4), :] = jnp.broadcast_to(
                mid[0, pl.ds(i, 1), pl.ds(c * 128, 128)], (4, 128)
            )
    changes = [
        0.2 * jnp.where(mine, wide[pl.ds(i * 24, 24), :], 0.0) - 0.4 * sums[i] for i in range(4)
    ]
    final[pl.ds(0, 96), :] = lanes_from(
        four_groups(jnp.concatenate(changes, axis=0)), lane_row // 4
    )

    everyone = squares * sizes[2]

    @pl.when(served)
    def _():
        whole = all_rows.at[pl.ds(1, everyone - 1)]
        remote(whole, whole, all_send.at[0], all_recv.at[0], here).wait_recv()
        all_rows[pl.ds(0, 1), :] = line_rows[pl.ds(0, 1), :]
        total_row[...] = jnp.sum(all_rows[...], axis=0, keepdims=True)

    @pl.when(jnp.logical_not(served))
    def _():
        plane_copies.arrived()
        total_row[...] = jnp.sum(plane_rows[...], axis=0, keepdims=True)

    totals = jnp.broadcast_to(total_row[...], (8, 128))
    totals = jnp.sum(jnp.where(lanes8 // 16 == rows8, totals, 0.0), axis=1, keepdims=True)
    first_norm, second_norm, cross_re, cross_im, ar, ai, br, bi = (
        jnp.broadcast_to(totals[i:i + 1, :], (1, 128)) for i in range(8)
    )
    determinant = first_norm * second_norm - cross_re * cross_re - cross_im * cross_im
    one_r = (second_norm * ar - (cross_re * br - cross_im * bi)) / determinant
    one_i = (second_norm * ai - (cross_re * bi + cross_im * br)) / determinant
    two_r = (first_norm * br - (cross_re * ar + cross_im * ai)) / determinant
    two_i = (first_norm * bi - (cross_re * ai - cross_im * ar)) / determinant
    ur, ui, wr, wi = (final[pl.ds(i * 24, 24), :] for i in range(4))
    update_re = final[96:120, :] + (one_r * ur - one_i * ui) + (two_r * wr - two_i * wi)
    update_im = final[120:144, :] + (one_r * ui + one_i * ur) + (two_r * wi + two_i * wr)
    update_re = update_re.astype(BF16).astype(F32)
    update_im = update_im.astype(BF16).astype(F32)
    for s in range(4):
        for c in range(3):
            vr, vi = fine_vector(0, s, c), fine_vector(1, s, c)
            add_re = jnp.sum(vr * update_re - vi * update_im, axis=0, keepdims=True)
            add_im = jnp.sum(vr * update_im + vi * update_re, axis=0, keepdims=True)
            row = s * 3 + c
            sol_ref[pl.ds(row, 1), :] = second[pl.ds(row, 1), :] + add_re
            sol_ref[pl.ds(12 + row, 1), :] = second[pl.ds(12 + row, 1), :] + add_im

    for group in (
        first_copies, second_copies, blk_copies, right_copies, line_copies, mid_copies,
        mid_line_copies,
    ):
        group.sent()
    left_out = sum((square >= 0).astype(jnp.int32) for square in spared)
    for n in range(len(targets) + 1):

        @pl.when(left_out == n)
        def _(n=n):
            whole = plane_rows.at[pl.ds(1, squares - 1 - n)]
            remote(whole, whole, plane_send, plane_recv, here).wait_send()

    for target, mine in zip(targets, chosen):

        @pl.when(jnp.logical_not(mine))
        def _(target=target):
            copy_to(target).wait_send()


def deliver(sol_v, res_v, sol_h, res_h, sem):
    copies = (
        pltpu.make_async_copy(sol_v, sol_h, sem.at[0]),
        pltpu.make_async_copy(res_v, res_h, sem.at[1]),
    )
    for copy in copies:
        copy.start()
    for copy in copies:
        copy.wait()


def solution(mesh):
    sizes = tuple(mesh.shape[axis] for axis in ("ta", "gz", "xy"))
    slots = plan(sizes)[1]

    def shards(source_field, gauge_links, fine_vectors, middle_blocks, middle_vectors, bottom_blocks):
        fine = jnp.transpose(fine_vectors, (0, 1, 3, 4, 5, 6, 2, 7)).reshape(576, 128)
        operands = (
            source_field.reshape(24, 128),
            gauge_links.reshape(144, 128),
            fine,
            middle_blocks.reshape(2592, 128),
            middle_vectors.reshape(288, 128),
            bottom_blocks.reshape(-1, 1, 128),
        )
        vmem = [pltpu.VMEM(o.shape, o.dtype) for o in operands]
        dma = pltpu.SemaphoreType.DMA
        sol, res = pl.pallas_call(
            functools.partial(kernel, sizes),
            out_shape=(pltpu.VMEM((24, 128), F32),) * 2,
            in_specs=[pl.BlockSpec(memory_space=pltpu.HBM)] * len(operands),
            out_specs=(pl.BlockSpec(memory_space=pltpu.VMEM),) * 2,
            scratch_shapes=vmem
            + [
                pltpu.VMEM((2, 8, 12, 128), F32),
                pltpu.VMEM((2, 6, 12, 128), F32),
                pltpu.VMEM((24, 128), F32),
                pltpu.VMEM((24, 128), F32),
                pltpu.VMEM((24, 128), F32),
                pltpu.VMEM((576, 128), F32),
                pltpu.VMEM((2, 2, 32, 768), BF16),
                pltpu.VMEM((1, 2, 6, 8, 128), F32),
                pltpu.VMEM((4, 2, 6, 8, 128), F32),
                pltpu.VMEM((2, 6, 56, 128), F32),
                pltpu.VMEM((len(slots), 128), F32),
                pltpu.VMEM((64, 128), F32),
                pltpu.VMEM((56, 128), F32),
                pltpu.VMEM((sizes[0] * sizes[1], 128), F32),
                pltpu.VMEM((sizes[2], 128), F32),
                pltpu.VMEM((9, 4, 768), F32),
                pltpu.VMEM((96, 128), F32),
                pltpu.VMEM((144, 128), F32),
                dma((len(operands),)),
                dma((2,)),
                dma((2,)),
            ]
            + [dma] * 12
            + [pltpu.SemaphoreType.REGULAR] * 2
            + [
                pltpu.VMEM((sizes[0] * sizes[1] * sizes[2], 128), F32),
                pltpu.VMEM((1, 128), F32),
                dma((1,)),
                dma((1,)),
            ],
            compiler_params=pltpu.CompilerParams(collective_id=0, has_side_effects=True),
        )(*operands)
        sol, res = pl.pallas_call(
            deliver,
            out_shape=(jax.ShapeDtypeStruct((24, 128), F32),) * 2,
            in_specs=[pl.BlockSpec(memory_space=pltpu.VMEM)] * 2,
            out_specs=(pl.BlockSpec(memory_space=pltpu.HBM),) * 2,
            scratch_shapes=[pltpu.SemaphoreType.DMA((2,))],
        )(*(pltpu.with_memory_space_constraint(o, pltpu.VMEM) for o in (sol, res)))
        return sol.reshape(source_field.shape), res.reshape(source_field.shape)

    return jax.shard_map(
        shards,
        mesh=mesh,
        in_specs=(
            P(None, None, None, "ta", "gz", "xy", None),
            P(None, None, None, None, "ta", "gz", "xy", None),
            P(None, None, None, None, "ta", "gz", "xy", None),
            P(None, None, None, "ta", "gz", "xy", None),
            P(None, None, "ta", "gz", "xy", None),
            P(None, None, "ta", "gz", None),
        ),
        out_specs=(
            P(None, None, None, "ta", "gz", "xy", None),
            P(None, None, None, "ta", "gz", "xy", None),
        ),
        check_vma=False,
    )
```
